512 devices in a mesh: dp: 64 (over z, y_lo, core), tensor: 8 (over x, y_hi).
Axes of the slice: x: 4, y: 8 (y_hi: 2, y_lo: 4; y = y_hi * 4 + y_lo), z: 8, core: 2. Of those that a mesh axis runs over, the one named last changes fastest.
Arguments:
- attn_out: bfloat16 [49152, 2048], P('dp', 'tensor'), may hold values from -6 to 6
- out_proj_t: bfloat16 [4096, 2048], P(None, 'tensor'), may hold values from -0.09375 to 0.09375
- grad_out: bfloat16 [49152, 4096], P('dp', 'tensor'), may hold values from -16 to 16
- read_weights: float32 [49152, 16], P('dp'), may hold values from 0 to 0.0026041667
- memory_gate: float32 [1024, 16], P('dp'), may hold values from -0.2 to 1
- write_pos: int32 [64, 16], P('dp'), may hold values from 0 to 767, as said below
Outputs:
- grad_attn_out: bfloat16 [49152, 2048], P('dp', 'tensor')
- grad_out_proj_t: float32 [4096, 2048], P('dp', 'tensor')
- grad_memory: float32 [1024, 4096], P('dp', 'tensor')
The draws below stay inside these ranges and needn't reach their ends.
Inputs may be any that keep to these rules, and one draw needn't show every extreme that they name: `write_pos`: the 16 positions of one segment are distinct.
All inputs are finite; a program needn't handle non-finite values.
Results may differ from the reference program's by a relative error of at most 0.0034.
Values may be sent and summed in bfloat16 or wider, within the bound.
A program may use at most 64 MiB of HBM per device.

```python
import jax
import jax.numpy as jnp
from jax import lax

D = 4096
MEM = 16
SEG = 768
SEGMENT_COUNT = 64
HD = 2048
TOKENS = 49152


def draw_memory_gate(key, part):
    share = 0.5
    gradual_decay = jax.random.uniform(jax.random.fold_in(key, 1), (1, MEM)) < share
    gradual_decay_rate = jnp.exp(-jax.random.uniform(jax.random.fold_in(key, 2), (SEGMENT_COUNT, MEM), jnp.float32, 0.2, 1.5) / SEGMENT_COUNT)
    quick_decay_rate = jax.random.uniform(jax.random.fold_in(key, 3), (SEGMENT_COUNT, MEM), jnp.float32, 0.05, 0.5)
    sudden_spike = jax.random.uniform(jax.random.fold_in(key, 4), (SEGMENT_COUNT, 1)) < 3.0 / SEGMENT_COUNT
    decay_rates = jnp.where(gradual_decay, gradual_decay_rate, quick_decay_rate) * jnp.where(sudden_spike, 0.6, 1.0)
    eye = jnp.eye(MEM, dtype=jnp.float32)
    spread = jnp.clip(jax.random.normal(jax.random.fold_in(key, 5), (SEGMENT_COUNT, MEM, MEM)) * 0.04, -0.2, 0.2)
    gates = spread * (1.0 - eye) + decay_rates[:, :, None] * eye
    return gates.reshape(SEGMENT_COUNT * MEM, MEM).astype(jnp.float32)


def draw_write_pos(key, part):
    keys = jax.random.split(jax.random.fold_in(key, 7), SEGMENT_COUNT)
    picks = jax.vmap(lambda single: jax.random.permutation(single, SEG)[:MEM])(keys)
    return picks.astype(jnp.int32)


def spiked(drawn, stream_key, source, target, parts, factor):
    def block_of(position):
        return (jnp.arange(drawn.shape[position]) // (drawn.shape[position] // parts)).reshape((-1,) + (1,) * (drawn.ndim - 1 - position))

    one_side = jax.random.permutation(stream_key, parts)[block_of(target)]
    second = (block_of(target) + parts // 2) % parts
    return jnp.where((block_of(source) == one_side) | (block_of(source) == second), factor * drawn, drawn)


def levels(rng, dims, cuts, low, high):
    def one(dim, shards_of):
        steps = jax.random.uniform(jax.random.fold_in(jax.random.fold_in(rng, 6), dim), (shards_of,), jnp.float32, low / len(cuts), high / len(cuts))
        return jnp.repeat(jnp.exp(steps), dims[dim] // shards_of).reshape((-1,) + (1,) * (len(dims) - dim - 1))

    factor_of = one(*cuts[0])
    for cut in cuts[1:]:
        factor_of = factor_of * one(*cut)
    return factor_of


def noise(own_key, extent, scale, reach, pieces=(), kind=jnp.bfloat16):
    drawn = scale * jax.random.normal(own_key, extent, jnp.float32)
    if pieces:
        drawn = drawn * levels(own_key, extent, pieces, -0.22, 0.18)
    return jnp.clip(drawn, -reach, reach).astype(kind)


def heavy_noise(own_key, shape, width, most, pieces, heavy, held_as=jnp.bfloat16):
    array = width * jax.random.normal(own_key, shape, jnp.float32)
    if pieces:
        array = array * levels(own_key, shape, pieces, -0.22, 0.18)
    return jnp.clip(spiked(array, jax.random.fold_in(own_key, 3), *heavy), -most, most).astype(held_as)


def setup_inputs(seed: int = 0) -> dict:
    seeds = jax.random.split(jax.random.key(seed), 7)
    attn_out = noise(seeds[0], (TOKENS, HD), 1.0, 6.0, ((0, 64), (1, 8)))
    out_proj_t = noise(seeds[1], (D, HD), D ** -0.5, 0.09375, ((1, 8),))
    grad_out = heavy_noise(seeds[2], (TOKENS, D), 1.0, 16.0, ((0, 64), (1, 8)), (0, 1, 64, 4.0))
    read_weights = jnp.clip(0.0026041667 * jax.random.uniform(seeds[3], (TOKENS, MEM), jnp.float32) ** levels(seeds[3], (TOKENS, MEM), ((0, 64),), -0.2, 0.2), 0.0, 0.0026041667)
    memory_gate = draw_memory_gate(jax.random.fold_in(seeds[6], 71), 0)
    write_pos = draw_write_pos(jax.random.fold_in(seeds[6], 71), 0)
    return {"attn_out": attn_out, "out_proj_t": out_proj_t, "grad_out": grad_out, "read_weights": read_weights, "memory_gate": memory_gate, "write_pos": write_pos}


def reference(attn_out, out_proj_t, grad_out, read_weights, memory_gate, write_pos):
    high = lax.Precision.HIGHEST
    dy = grad_out.astype(jnp.float32).reshape(SEGMENT_COUNT, SEG, D)
    reads = read_weights.reshape(SEGMENT_COUNT, SEG, MEM)
    gates = memory_gate.reshape(SEGMENT_COUNT, MEM, MEM)
    local = jnp.einsum('stm,std->smd', reads, dy, precision=high)

    def sweep(carry, inputs):
        gate, term = inputs
        fresh = jnp.dot(gate.T, carry, precision=high, preferred_element_type=jnp.float32) + term
        return fresh, (fresh, carry)

    start = jnp.zeros((MEM, D), jnp.float32)
    _, (grad_mem, after) = lax.scan(sweep, start, (gates, local), reverse=True)
    places = jnp.arange(SEG, dtype=jnp.int32)
    onehot = (places[None, :, None] == write_pos[:, None, :]).astype(jnp.float32)
    written = jnp.einsum('stm,smd->std', onehot, after, precision=high)
    grad_z = (dy + written).astype(jnp.bfloat16).reshape(TOKENS, D)
    grad_attn = jnp.dot(grad_z, out_proj_t, preferred_element_type=jnp.float32).astype(jnp.bfloat16)
    grad_weight = lax.dot_general(grad_z, attn_out, (((0,), (0,)), ((), ())), preferred_element_type=jnp.float32)
    return grad_attn, grad_weight, grad_mem.reshape(SEGMENT_COUNT * MEM, D)
```

```python
import functools

import jax
import jax.numpy as jnp
from jax import lax
from jax.experimental import pallas as pl
from jax.experimental.pallas import tpu as pltpu
from jax.sharding import PartitionSpec as P

T, DS, HS, MEM = 768, 512, 256, 16
XCH, XROWS = 3, 256
YCH, YROWS = 4, 192
F32, BF16 = jnp.float32, jnp.bfloat16
HIGH = lax.Precision.HIGHEST
SUM0 = (((0,), (0,)), ((), ()))


def tdot(a, b, precision=None):
    return lax.dot_general(a, b, SUM0, precision=precision, preferred_element_type=F32)


def dot(a, b):
    return jnp.dot(a, b, preferred_element_type=F32)


def parts3(v):
    hi = v.astype(BF16)
    rest = v - hi.astype(F32)
    mid = rest.astype(BF16)
    return hi, mid, (rest - mid.astype(F32)).astype(BF16)


def apply_map(m, v):
    out = m[:, 0:1] * v[0:1, :]
    for k in range(1, MEM):
        out = out + m[:, k : k + 1] * v[k : k + 1, :]
    return out


def kernel(
    g, attn, w, rw, gate, wp, oa, ow, om,
    G, A, ARelay, WP, S1, S2, S3, vr, R, Rows, acc, Ps, PRelay, Pr, Pf, Cs, Cr, Ss, Zr, Ys, Yr, oh,
    xs, xr, fs, fr, as1, ar1, as2, ar2, w1, wzs, wzr, wc, l1, l2s, l2r, l3s, l3r, rs, rr,
    ps1, pr1, ps2, pr2, cs, cr, zs, zr, ys, yr,
):
    dp, tp = lax.axis_index("dp"), lax.axis_index("tensor")
    z, yl, c = lax.div(dp, 8), lax.rem(lax.div(dp, 2), 4), lax.rem(dp, 2)
    x, yh = lax.div(tp, 2), lax.rem(tp, 2)
    y = 4 * yh + yl

    def dev(x_=None, y_=None, z_=None, c_=None):
        x_ = x if x_ is None else x_
        y_ = y if y_ is None else y_
        z_ = z if z_ is None else z_
        c_ = c if c_ is None else c_
        return (8 * z_ + 2 * lax.rem(y_, 4) + c_, 2 * x_ + lax.div(y_, 4))

    def copy(src, dst, send, recv, to):
        return pltpu.make_async_remote_copy(
            src_ref=src, dst_ref=dst, send_sem=send, recv_sem=recv,
            device_id=to, device_id_type=pl.DeviceIdType.MESH,
        )

    xn = [lax.rem(x + k, 4) for k in range(4)]
    right, left, across = dev(x_=xn[1]), dev(x_=xn[3]), dev(x_=xn[2])
    yn = [lax.rem(y + k, 8) for k in range(8)]
    up, down, far = dev(y_=yn[2]), dev(y_=yn[6]), dev(y_=yn[4])
    mate = dev(c_=1 - c)
    lo = [dev(y_=4 * yh + lax.rem(yl + k, 4)) for k in range(4)]
    zn = [lax.rem(z + k, 8) for k in range(8)]
    zdev = [dev(z_=zn[k]) for k in range(8)]
    odd = lax.rem(z, 2)
    zx = z + 1 - 2 * odd
    straight = odd == yh
    cross = [dev(y_=4 * (1 - yh) + lax.rem(yl + k, 4), z_=zx) for k in range(4)]

    barrier = pltpu.get_barrier_semaphore()
    greeted = [right, left, across, up, down, far, mate] + lo[1:] + zdev[1:] + cross
    for peer in greeted:
        pl.semaphore_signal(barrier, inc=1, device_id=peer, device_id_type=pl.DeviceIdType.MESH)
    pl.semaphore_wait(barrier, len(greeted))

    sent = []

    def go(d):
        d.start()
        sent.append(d)

    def own_right(k):
        r = pl.ds(k * XROWS, XROWS)
        return copy(g.at[r], G.at[2, r], xs.at[0, k], xr.at[0, k], right)

    def own_left(k):
        r = pl.ds(k * XROWS, XROWS)
        return copy(g.at[r], G.at[0, r], xs.at[1, k], xr.at[1, k], left)

    half = XROWS // 2

    def on_right(k):
        r = pl.ds(k * XROWS, half)
        return copy(G.at[2, r], G.at[1, r], fs.at[0, k], fr.at[0, k], right)

    def on_left(k):
        r = pl.ds(k * XROWS + half, half)
        return copy(G.at[0, r], G.at[1, r], fs.at[1, k], fr.at[1, k], left)

    def ydir(j):
        return up if j < YCH // 2 else down

    def attn_first(j):
        r = pl.ds(j * YROWS, YROWS)
        return copy(attn.at[r], ARelay.at[j], as1.at[j], ar1.at[j], ydir(j))

    def attn_second(j):
        origin = yn[6] if j < YCH // 2 else yn[2]
        cols = pl.ds(pl.multiple_of(lax.div(origin, 4) * HS, HS), HS)
        r = pl.ds(j * YROWS, YROWS)
        return copy(ARelay.at[j], A.at[r, cols], as2.at[j], ar2.at[j], ydir(j))

    for k in range(XCH):
        go(own_right(k))
        go(own_left(k))
    go(attn_first(0))
    go(attn_first(2))
    wrow = pl.multiple_of((2 * (2 * c + lax.div(z, 4)) + 1 - yh) * DS + lax.rem(z, 4) * 128, 128)
    wpiece = pl.ds(pl.multiple_of(c * 1024 + z * 128, 128), 128)
    wfirst = copy(w.at[pl.ds(wrow, 128)], WP.at[wpiece], w1.at[0], w1.at[1], far)
    go(wfirst)

    picks = lax.broadcasted_iota(jnp.int32, (T, MEM), 0) == wp[...]
    oh[...] = picks.astype(F32).astype(BF16)
    gv = g[...]
    hi, mid, low = parts3(rw[...])
    local = tdot(low, gv) + tdot(mid, gv) + tdot(hi, gv)
    eye = (
        lax.broadcasted_iota(jnp.int32, (MEM, 128), 0)
        == lax.broadcasted_iota(jnp.int32, (MEM, 128), 1)
    ).astype(F32)
    S1[c, :, :DS] = local
    S1[c, :, DS:] = tdot(gate[...], eye, HIGH)
    lcopy = copy(S1.at[c], S1.at[c], l1.at[0], l1.at[1], mate)
    go(lcopy)
    grows = tdot(oh[...], gv)
    own_cols = pl.ds(pl.multiple_of(yh * HS, HS), HS)
    A[:, own_cols] = attn[...]

    def compose(early, late):
        both = apply_map(early[:, DS:], late)
        return both[:, :DS] + early[:, :DS], both[:, DS:]

    lcopy.wait_recv()
    term, mat = compose(S1[0], S1[1])
    S2[yl, :, :DS] = term
    S2[yl, :, DS:] = mat
    for k in range(1, 4):
        go(copy(S2.at[yl], S2.at[yl], l2s.at[k], l2r.at[yl], lo[k]))
    go(attn_first(1))
    go(attn_first(3))
    for k in range(1, 4):
        slot = lax.rem(yl + k, 4)
        copy(S2.at[slot], S2.at[slot], l2s.at[k], l2r.at[slot], lo[k]).wait_recv()
    term, mat = compose(S2[2], S2[3])
    for k in (1, 0):
        term, mat = compose(S2[k], jnp.concatenate([term, mat], axis=1))
    S3[z, :, :DS] = term
    S3[z, :, DS:] = mat
    for zz in range(7):
        @pl.when(zz < z)
        def _():
            copy(S3.at[z], S3.at[z], l3s.at[zz], l3r.at[z], dev(z_=zz)).start()

    for j in (0, 2):
        attn_first(j).wait_recv()
        go(attn_second(j))
    wfirst.wait_recv()

    def wspread(k):
        piece = pl.ds(pl.multiple_of(c * 1024 + zn[k] * 128, 128), 128)
        return copy(WP.at[piece], WP.at[piece], wzs.at[k], wzr.at[zn[k]], zdev[k])

    for k in (1, 7, 2, 6, 3, 5, 4):
        go(copy(WP.at[wpiece], WP.at[wpiece], wzs.at[k], wzr.at[z], zdev[k]))
    for j in (1, 3):
        attn_first(j).wait_recv()
        go(attn_second(j))

    vr[...] = jnp.zeros((MEM, DS), F32)

    def through(s):
        vr[...] = apply_map(s[:, DS:], vr[...]) + s[:, :DS]

    for zz in range(7, 0, -1):
        @pl.when(zz > z)
        def _():
            copy(S3.at[zz], S3.at[zz], l3s.at[0], l3r.at[zz], dev(z_=zz)).wait_recv()
            through(S3[zz])

    for k in range(3, 0, -1):
        @pl.when(k > yl)
        def _():
            through(S2[k])

    @pl.when(c == 0)
    def _():
        through(S1[1])

    after = vr[...]
    mine = S1[c]
    om[...] = apply_map(mine[:, DS:], after) + mine[:, :DS]
    R[0, :MEM] = (grows + after).astype(BF16)
    R[0, MEM:] = (-grows).astype(BF16)

    def rcopy(k):
        return copy(R.at[0], R.at[4 - k], rs.at[k], rr.at[4 - k], (right, across, left)[k - 1])

    for k in (1, 3, 2):
        go(rcopy(k))
    for k in range(XCH):
        own_right(k).wait_recv()
        go(on_right(k))
        own_left(k).wait_recv()
        go(on_left(k))
    for k in range(1, 8):
        wspread(k).wait_recv()
    chalf = pl.ds(pl.multiple_of(c * 1024, 1024), 1024)
    ohalf = pl.ds(pl.multiple_of((1 - c) * 1024, 1024), 1024)
    go(copy(WP.at[chalf], WP.at[chalf], wc.at[0], wc.at[1], mate))

    def rows_of(rel):
        return g if rel == 0 else G.at[rel - 1]

    def forward(rel, which, first):
        src = rows_of(rel)
        if which == 0:
            weight = w[pl.ds(pl.multiple_of((2 * xn[rel] + yh) * DS, DS), DS), :]
        else:
            weight = WP[pl.ds(pl.multiple_of(xn[rel] * DS, DS), DS), :]
        for b in range(3):
            r = pl.ds(b * 256, 256)
            part = dot(src[r, :], weight)
            acc[which, r, :] = part if first else acc[which, r, :] + part

    def gradient(rel):
        src = rows_of(rel)
        for b in range(2):
            cols = pl.ds(b * 256, 256)
            Pf[rel, cols, :] = tdot(src[:, cols], A[...]) + tdot(R[rel, :, cols], Rows[...])
        for k in range(4):
            theirs = pl.ds(pl.multiple_of((2 * k + 1 - c) * 64, 64), 64)
            Cs[rel, k * 64 : k * 64 + 64, :] = Pf[rel, theirs, :].astype(BF16)
        go(ccopy(rel))

    def ccopy(rel):
        return copy(Cs.at[rel], Cr.at[rel], cs.at[rel], cr.at[rel], mate)

    def zsend(rel, q):
        return copy(
            Ss.at[rel, q], Zr.at[z], zs.at[rel, q], zr.at[z], dev(z_=2 * xn[rel] + q)
        )

    def scatter(rel):
        ccopy(rel).wait_recv()
        for k in range(4):
            ours = pl.ds(pl.multiple_of((2 * k + c) * 64, 64), 64)
            part = slice(k * 64, k * 64 + 64)
            total = (Pf[rel, ours, :] + Cr[rel, part, :].astype(F32)).astype(BF16)
            Ss[rel, 0, part, :] = total[:, :HS]
            Ss[rel, 1, part, :] = total[:, HS:]
        for q in range(2):
            @pl.when(2 * xn[rel] + q != z)
            def _():
                zsend(rel, q).start()

            @pl.when(2 * xn[rel] + q == z)
            def _():
                Zr[z] = Ss[rel, q]

    forward(0, 0, True)
    for j in range(YCH):
        attn_second(j).wait_recv()
    arows = tdot(oh[...], A[...]).astype(BF16)
    Rows[:MEM] = arows
    Rows[MEM:] = arows
    gradient(0)
    copy(WP.at[ohalf], WP.at[ohalf], wc.at[0], wc.at[1], mate).wait_recv()
    forward(0, 1, True)
    scatter(0)
    for k in (3, 1):
        rcopy(k).wait_recv()
        gradient(4 - k)
        forward(4 - k, 0, False)
        forward(4 - k, 1, False)
        scatter(4 - k)
    rcopy(2).wait_recv()
    for k in range(XCH):
        on_right(k).wait_recv()
        on_left(k).wait_recv()
    forward(2, 1, False)

    def change(which):
        total = None
        for rel in range(4):
            if which == 0:
                weight = w[pl.ds(pl.multiple_of((2 * xn[rel] + yh) * DS, DS), DS), :]
            else:
                weight = WP[pl.ds(pl.multiple_of(xn[rel] * DS, DS), DS), :]
            part = dot(R[rel], weight)
            total = part if total is None else total + part
        hi, mid, low = parts3(total[:MEM] + total[MEM:])
        o = oh[...]
        return dot(o, hi) + dot(o, mid) + dot(o, low)

    Ps[...] = (acc[1] + change(1)).astype(BF16)

    def part_first(j):
        r = pl.ds(j * YROWS, YROWS)
        return copy(Ps.at[r], PRelay.at[j], ps1.at[j], pr1.at[j], ydir(j))

    def part_second(j):
        r = pl.ds(j * YROWS, YROWS)
        return copy(PRelay.at[j], Pr.at[r], ps2.at[j], pr2.at[j], ydir(j))

    gradient(2)
    for j in (0, 2, 1, 3):
        go(part_first(j))
    scatter(2)
    forward(2, 0, False)
    acc[0] = acc[0] + change(0)
    for j in (0, 2, 1, 3):
        part_first(j).wait_recv()
        go(part_second(j))

    for zz in range(8):
        @pl.when(zz != z)
        def _():
            copy(Zr.at[zz], Zr.at[zz], zs.at[0, 0], zr.at[zz], dev(z_=zz)).wait_recv()

    total = Zr[0].astype(F32)
    for zz in range(1, 8):
        total = total + Zr[zz].astype(F32)
    for k in range(4):
        Ys[k] = total[k * 64 : k * 64 + 64].astype(BF16)

    zf = jnp.where(straight, z, zx)
    yhf = jnp.where(straight, yh, 1 - yh)

    def ysend(k):
        there = lax.rem(yl + k, 4)
        return copy(Ys.at[there], Yr.at[yl], ys.at[k], yr.at[yl], dev(y_=4 * yhf + there, z_=zf))

    for k in range(1, 4):
        go(ysend(k))

    @pl.when(straight)
    def _():
        Yr[yl] = Ys[yl]

    @pl.when(jnp.logical_not(straight))
    def _():
        ysend(0).start()

    for j in (0, 2, 1, 3):
        part_second(j).wait_recv()
    oa[...] = (acc[0] + Pr[...].astype(F32)).astype(BF16)

    for k in range(1, 4):
        slot = lax.rem(yl + k, 4)
        copy(Ys.at[0], Yr.at[slot], ys.at[k], yr.at[slot], lo[k]).wait_recv()

    @pl.when(jnp.logical_not(straight))
    def _():
        d = ysend(0)
        d.wait_send()
        d.wait_recv()

    ow[...] = (Yr[0].astype(F32) + Yr[1].astype(F32)) + (Yr[2].astype(F32) + Yr[3].astype(F32))

    for d in sent:
        d.wait_send()
    for zz in range(7):
        @pl.when(zz < z)
        def _():
            copy(S3.at[z], S3.at[z], l3s.at[zz], l3r.at[z], dev(z_=zz)).wait_send()
    for rel in range(4):
        for q in range(2):
            @pl.when(2 * xn[rel] + q != z)
            def _():
                zsend(rel, q).wait_send()


def body(attn_out, out_proj_t, grad_out, read_weights, memory_gate, write_pos):
    vm = pl.BlockSpec(memory_space=pltpu.VMEM)
    V, D = pltpu.VMEM, pltpu.SemaphoreType.DMA
    scratch = [
        V((3, T, DS), BF16), V((T, 2 * HS), BF16), V((YCH, YROWS, HS), BF16), V((2048, HS), BF16),
        V((2, MEM, DS + 128), F32), V((4, MEM, DS + 128), F32), V((8, MEM, DS + 128), F32),
        V((MEM, DS), F32), V((4, 2 * MEM, DS), BF16), V((2 * MEM, 2 * HS), BF16),
        V((2, T, HS), F32), V((T, HS), BF16), V((YCH, YROWS, HS), BF16), V((T, HS), BF16),
        V((4, DS, 2 * HS), F32), V((4, 256, 2 * HS), BF16), V((4, 256, 2 * HS), BF16),
        V((4, 2, 256, HS), BF16), V((8, 256, HS), BF16), V((4, 64, HS), BF16), V((4, 64, HS), BF16),
        V((T, MEM), BF16),
        D((2, XCH)), D((2, XCH)), D((2, XCH)), D((2, XCH)),
        D((YCH,)), D((YCH,)), D((YCH,)), D((YCH,)),
        D((2,)), D((8,)), D((8,)), D((2,)), D((2,)), D((4,)), D((4,)), D((8,)), D((8,)),
        D((4,)), D((4,)), D((YCH,)), D((YCH,)), D((YCH,)), D((YCH,)),
        D((4,)), D((4,)), D((4, 2)), D((8,)), D((4,)), D((4,)),
    ]
    return pl.pallas_call(
        kernel,
        out_shape=(
            jax.ShapeDtypeStruct((T, HS), BF16),
            jax.ShapeDtypeStruct((64, HS), F32),
            jax.ShapeDtypeStruct((MEM, DS), F32),
        ),
        in_specs=[vm] * 6,
        out_specs=(vm,) * 3,
        scratch_shapes=scratch,
        compiler_params=pltpu.CompilerParams(
            collective_id=0, has_side_effects=True, vmem_limit_bytes=60 * 1024 * 1024
        ),
    )(grad_out, attn_out, out_proj_t, read_weights, memory_gate, write_pos)


def solution(mesh):
    placed = (
        P("dp", "tensor"), P(None, "tensor"), P("dp", "tensor"),
        P("dp", None), P("dp", None), P("dp", None),
    )
    return jax.shard_map(
        body, mesh=mesh, in_specs=placed,
        out_specs=(P("dp", "tensor"), P("dp", "tensor"), P("dp", "tensor")), check_vma=False,
    )
```

```python
import functools

import jax
import jax.numpy as jnp
from jax import lax
from jax.experimental import pallas as pl
from jax.experimental.pallas import tpu as pltpu
from jax.sharding import PartitionSpec as P

T, DS, HS, MEM = 768, 512, 256, 16
XCH, XROWS = 3, 256
YCH, YROWS = 3, 256
F32, BF16 = jnp.float32, jnp.bfloat16
HIGH = lax.Precision.HIGHEST
SUM0 = (((0,), (0,)), ((), ()))


def tdot(a, b, precision=None):
    return lax.dot_general(a, b, SUM0, precision=precision, preferred_element_type=F32)


def dot(a, b):
    return jnp.dot(a, b, preferred_element_type=F32)


def parts3(v):
    hi = v.astype(BF16)
    rest = v - hi.astype(F32)
    mid = rest.astype(BF16)
    return hi, mid, (rest - mid.astype(F32)).astype(BF16)


def apply_map(m, v):
    out = m[:, 0:1] * v[0:1, :]
    for k in range(1, MEM):
        out = out + m[:, k : k + 1] * v[k : k + 1, :]
    return out


def kernel(
    g_in, attn, w_in, rwt_in, gate_in, wp_in, oa, ow, om,
    g, w, rwt, gate, wp, G, A, WP, S1, S2, S3, vr, R, Rows, acc, Ps, Pr, Pf, Cs, Cr, Ss, Zr, Ys, Yr, oh,
    ins, xs, xr, fs, fr, ats, atr, w1, wzs, wzr, wc, l1, l2s, l2r, l3s, l3r, rs, rr,
    ps, pr, cs, cr, zs, zr, ys, yr,
):
    dp, tp = lax.axis_index("dp"), lax.axis_index("tensor")
    z, yl, c = lax.div(dp, 8), lax.rem(lax.div(dp, 2), 4), lax.rem(dp, 2)
    x, yh = lax.div(tp, 2), lax.rem(tp, 2)
    y = 4 * yh + yl

    def dev(x_=None, y_=None, z_=None, c_=None):
        x_ = x if x_ is None else x_
        y_ = y if y_ is None else y_
        z_ = z if z_ is None else z_
        c_ = c if c_ is None else c_
        return (8 * z_ + 2 * lax.rem(y_, 4) + c_, 2 * x_ + lax.div(y_, 4))

    def copy(src, dst, send, recv, to):
        return pltpu.make_async_remote_copy(
            src_ref=src, dst_ref=dst, send_sem=send, recv_sem=recv,
            device_id=to, device_id_type=pl.DeviceIdType.MESH,
        )

    xn = [lax.rem(x + k, 4) for k in range(4)]
    right, left, across = dev(x_=xn[1]), dev(x_=xn[3]), dev(x_=xn[2])
    yn = [lax.rem(y + k, 8) for k in range(8)]
    far = dev(y_=yn[4])
    mate = dev(c_=1 - c)
    lo = [dev(y_=4 * yh + lax.rem(yl + k, 4)) for k in range(4)]
    zn = [lax.rem(z + k, 8) for k in range(8)]
    zdev = [dev(z_=zn[k]) for k in range(8)]
    odd = lax.rem(z, 2)
    zx = z + 1 - 2 * odd
    straight = odd == yh
    cross = [dev(y_=4 * (1 - yh) + lax.rem(yl + k, 4), z_=zx) for k in range(4)]

    barrier = pltpu.get_barrier_semaphore()
    greeted = [right, left, across, far, mate] + lo[1:] + zdev[1:] + cross
    for peer in greeted:
        pl.semaphore_signal(barrier, inc=1, device_id=peer, device_id_type=pl.DeviceIdType.MESH)

    loads = [
        pltpu.make_async_copy(wp_in, wp, ins.at[6]),
        pltpu.make_async_copy(gate_in, gate, ins.at[7]),
        pltpu.make_async_copy(rwt_in, rwt, ins.at[8]),
        pltpu.make_async_copy(g_in, g, ins.at[0]),
        pltpu.make_async_copy(attn, A.at[0], ins.at[1]),
    ]
    for k in range(4):
        block = pl.ds(pl.multiple_of((2 * k + yh) * DS, DS), DS)
        loads.append(pltpu.make_async_copy(w_in.at[block], w.at[pl.ds(k * DS, DS)], ins.at[2 + k]))
    for load in loads:
        load.start()

    loads[0].wait()
    picks = lax.broadcasted_iota(jnp.int32, (T, MEM), 0) == wp[...]
    oh[...] = picks.astype(F32).astype(BF16)
    eye = (
        lax.broadcasted_iota(jnp.int32, (MEM, 128), 0)
        == lax.broadcasted_iota(jnp.int32, (MEM, 128), 1)
    ).astype(F32)
    loads[1].wait()
    S1[c, :, DS:] = tdot(gate[...], eye, HIGH)
    loads[2].wait()
    hi, mid, low = parts3(rwt[...])
    loads[3].wait()
    gv = g[...]
    S1[c, :, :DS] = dot(low, gv) + dot(mid, gv) + dot(hi, gv)
    pl.semaphore_wait(barrier, len(greeted))

    sent = []

    def go(d):
        d.start()
        sent.append(d)

    lcopy = copy(S1.at[c], S1.at[c], l1.at[0], l1.at[1], mate)
    go(lcopy)

    def own_right(k):
        r = pl.ds(k * XROWS, XROWS)
        return copy(g.at[r], G.at[2, r], xs.at[0, k], xr.at[0, k], right)

    def own_left(k):
        r = pl.ds(k * XROWS, XROWS)
        return copy(g.at[r], G.at[0, r], xs.at[1, k], xr.at[1, k], left)

    half = XROWS // 2

    def on_right(k):
        r = pl.ds(k * XROWS, half)
        return copy(G.at[2, r], G.at[1, r], fs.at[0, k], fr.at[0, k], right)

    def on_left(k):
        r = pl.ds(k * XROWS + half, half)
        return copy(G.at[0, r], G.at[1, r], fs.at[1, k], fr.at[1, k], left)

    def attn_far(j):
        r = pl.ds(j * YROWS, YROWS)
        return copy(A.at[0, r], A.at[1, r], ats.at[j], atr.at[j], far)

    for k in range(XCH):
        go(own_right(k))
        go(own_left(k))
    part = lax.rem(z, 4)
    wrow = pl.multiple_of(
        (2 * (2 * c + lax.div(part, 2)) + 1 - yh) * DS + lax.rem(part, 2) * 256, 256
    )

    def wpart(k):
        return pl.ds(pl.multiple_of(c * 1024 + lax.rem(z + k, 4) * 256, 256), 256)

    wfirst = copy(w_in.at[pl.ds(wrow, 256)], WP.at[wpart(0)], w1.at[0], w1.at[1], far)

    def compose(early, late):
        both = apply_map(early[:, DS:], late)
        return both[:, :DS] + early[:, :DS], both[:, DS:]

    lcopy.wait_recv()
    term, mat = compose(S1[0], S1[1])
    S2[yl, :, :DS] = term
    S2[yl, :, DS:] = mat
    for k in range(1, 4):
        go(copy(S2.at[yl], S2.at[yl], l2s.at[k], l2r.at[yl], lo[k]))
    loads[4].wait()
    grows = tdot(oh[...], gv)
    for k in range(1, 4):
        slot = lax.rem(yl + k, 4)
        copy(S2.at[slot], S2.at[slot], l2s.at[k], l2r.at[slot], lo[k]).wait_recv()
    term, mat = compose(S2[2], S2[3])
    for k in (1, 0):
        term, mat = compose(S2[k], jnp.concatenate([term, mat], axis=1))
    S3[z, :, :DS] = term
    S3[z, :, DS:] = mat
    for zz in range(7):
        @pl.when(zz < z)
        def _():
            copy(S3.at[z], S3.at[z], l3s.at[zz], l3r.at[z], dev(z_=zz)).start()

    go(wfirst)
    for j in range(YCH):
        go(attn_far(j))

    vr[...] = jnp.zeros((MEM, DS), F32)

    def through(s):
        vr[...] = apply_map(s[:, DS:], vr[...]) + s[:, :DS]

    for zz in range(7, 0, -1):
        @pl.when(zz > z)
        def _():
            copy(S3.at[zz], S3.at[zz], l3s.at[0], l3r.at[zz], dev(z_=zz)).wait_recv()
            through(S3[zz])

    for k in range(3, 0, -1):
        @pl.when(k > yl)
        def _():
            through(S2[k])

    @pl.when(c == 0)
    def _():
        through(S1[1])

    after = vr[...]
    mine = S1[c]
    om[...] = apply_map(mine[:, DS:], after) + mine[:, :DS]
    R[0, :MEM] = (grows + after).astype(BF16)
    R[0, MEM:] = (-grows).astype(BF16)

    def rcopy(k):
        return copy(R.at[0], R.at[4 - k], rs.at[k], rr.at[4 - k], (right, across, left)[k - 1])

    for k in (1, 3, 2):
        go(rcopy(k))
    def rows_of(rel):
        return g if rel == 0 else G.at[rel - 1]

    def forward(rel, which, first):
        src = rows_of(rel)
        if which == 0:
            weight = w[pl.ds(pl.multiple_of(xn[rel] * DS, DS), DS), :]
        else:
            weight = WP[pl.ds(pl.multiple_of(xn[rel] * DS, DS), DS), :]
        for b in range(3):
            r = pl.ds(b * 256, 256)
            part = dot(src[r, :], weight)
            acc[which, r, :] = part if first else acc[which, r, :] + part

    qs = (yh, 1 - yh)

    def gradient(rel, h):
        src = rows_of(rel)
        for b in range(2):
            cols = pl.ds(b * 256, 256)
            Pf[rel, h, cols, :] = tdot(src[:, cols], A[h]) + tdot(R[rel, :, cols], Rows[h])
        for k in range(4):
            theirs = pl.ds(pl.multiple_of((2 * k + 1 - c) * 64, 64), 64)
            Cs[rel, h, k * 64 : k * 64 + 64, :] = Pf[rel, h, theirs, :].astype(BF16)
        go(ccopy(rel, h))

    def ccopy(rel, h):
        return copy(Cs.at[rel, h], Cr.at[rel, h], cs.at[rel, h], cr.at[rel, h], mate)

    def zsend(rel, h):
        to = dev(z_=2 * xn[rel] + qs[h])
        return copy(Ss.at[rel, h], Zr.at[z], zs.at[rel, h], zr.at[z], to)

    def scatter(rel, h):
        ccopy(rel, h).wait_recv()
        for k in range(4):
            ours = pl.ds(pl.multiple_of((2 * k + c) * 64, 64), 64)
            part = slice(k * 64, k * 64 + 64)
            total = Pf[rel, h, ours, :] + Cr[rel, h, part, :].astype(F32)
            Ss[rel, h, part, :] = total.astype(BF16)

        @pl.when(2 * xn[rel] + qs[h] != z)
        def _():
            zsend(rel, h).start()

        @pl.when(2 * xn[rel] + qs[h] == z)
        def _():
            Zr[z] = Ss[rel, h]

    def pick(h):
        arows = tdot(oh[...], A[h]).astype(BF16)
        Rows[h, :MEM] = arows
        Rows[h, MEM:] = arows

    wfirst.wait_recv()

    wto = [zdev[1], zdev[7], dev(z_=lax.rem(z + 2 + 4 * c, 8))]

    def wspread(k, piece):
        return copy(WP.at[wpart(piece)], WP.at[wpart(piece)], wzs.at[k], wzr.at[k], wto[k])

    for k in range(3):
        go(wspread(k, 0))
    pick(0)
    gradient(0, 0)
    for k in range(XCH):
        own_right(k).wait_recv()
        go(on_right(k))
        own_left(k).wait_recv()
        go(on_left(k))
    rcopy(1).wait_recv()
    gradient(3, 0)
    rcopy(3).wait_recv()
    gradient(1, 0)
    for k, piece in enumerate((3, 1, 2)):
        wspread(k, piece).wait_recv()
    chalf = pl.ds(pl.multiple_of(c * 1024, 1024), 1024)
    ohalf = pl.ds(pl.multiple_of((1 - c) * 1024, 1024), 1024)
    go(copy(WP.at[chalf], WP.at[chalf], wc.at[0], wc.at[1], mate))
    scatter(0, 0)
    scatter(3, 0)
    scatter(1, 0)
    for load in loads[5:]:
        load.wait()
    for rel in (0, 3, 1):
        forward(rel, 0, rel == 0)
    copy(WP.at[ohalf], WP.at[ohalf], wc.at[0], wc.at[1], mate).wait_recv()
    for rel in (0, 3, 1):
        forward(rel, 1, rel == 0)
    rcopy(2).wait_recv()

    def change(which):
        total = None
        for rel in range(4):
            if which == 0:
                weight = w[pl.ds(pl.multiple_of(xn[rel] * DS, DS), DS), :]
            else:
                weight = WP[pl.ds(pl.multiple_of(xn[rel] * DS, DS), DS), :]
            part = dot(R[rel], weight)
            total = part if total is None else total + part
        return parts3(total[:MEM] + total[MEM:])

    def spread(rows, change3):
        o = oh[rows, :]
        return dot(o, change3[0]) + dot(o, change3[1]) + dot(o, change3[2])

    def part_far(j):
        r = pl.ds(j * YROWS, YROWS)
        return copy(Ps.at[r], Pr.at[r], ps.at[j], pr.at[j], far)

    theirs = change(1)
    weight = WP[pl.ds(pl.multiple_of(xn[2] * DS, DS), DS), :]
    for j in range(YCH):
        on_right(j).wait_recv()
        on_left(j).wait_recv()
        r = pl.ds(j * YROWS, YROWS)
        Ps[r, :] = (acc[1, r, :] + dot(G[1, r, :], weight) + spread(r, theirs)).astype(BF16)
        go(part_far(j))
    gradient(2, 0)
    forward(2, 0, False)
    scatter(2, 0)
    for j in range(YCH):
        attn_far(j).wait_recv()
    pick(1)
    gradient(0, 1)
    gradient(3, 1)
    scatter(0, 1)
    gradient(1, 1)
    scatter(3, 1)
    gradient(2, 1)
    scatter(1, 1)
    scatter(2, 1)
    ours = change(0)
    for j in range(YCH):
        r = pl.ds(j * YROWS, YROWS)
        acc[0, r, :] = acc[0, r, :] + spread(r, ours)
    for zz in range(8):
        @pl.when(zz != z)
        def _():
            copy(Zr.at[zz], Zr.at[zz], zs.at[0, 0], zr.at[zz], dev(z_=zz)).wait_recv()

    total = Zr[0].astype(F32)
    for zz in range(1, 8):
        total = total + Zr[zz].astype(F32)
    for k in range(4):
        Ys[k] = total[k * 64 : k * 64 + 64].astype(BF16)

    zf = jnp.where(straight, z, zx)
    yhf = jnp.where(straight, yh, 1 - yh)

    def ysend(k):
        there = lax.rem(yl + k, 4)
        return copy(Ys.at[there], Yr.at[yl], ys.at[k], yr.at[yl], dev(y_=4 * yhf + there, z_=zf))

    for k in range(1, 4):
        go(ysend(k))

    @pl.when(straight)
    def _():
        Yr[yl] = Ys[yl]

    @pl.when(jnp.logical_not(straight))
    def _():
        ysend(0).start()

    for j in range(YCH):
        part_far(j).wait_recv()
    oa[...] = (acc[0] + Pr[...].astype(F32)).astype(BF16)

    for k in range(1, 4):
        slot = lax.rem(yl + k, 4)
        copy(Ys.at[0], Yr.at[slot], ys.at[k], yr.at[slot], lo[k]).wait_recv()

    @pl.when(jnp.logical_not(straight))
    def _():
        d = ysend(0)
        d.wait_send()
        d.wait_recv()

    ow[...] = (Yr[0].astype(F32) + Yr[1].astype(F32)) + (Yr[2].astype(F32) + Yr[3].astype(F32))

    for d in sent:
        d.wait_send()
    for zz in range(7):
        @pl.when(zz < z)
        def _():
            copy(S3.at[z], S3.at[z], l3s.at[zz], l3r.at[z], dev(z_=zz)).wait_send()
    for rel in range(4):
        for h in range(2):
            @pl.when(2 * xn[rel] + qs[h] != z)
            def _():
                zsend(rel, h).wait_send()


def finish(a, b, c, oa, ow, om):
    oa[...] = a[...]
    ow[...] = b[...]
    om[...] = c[...]


def body(attn_out, out_proj_t, grad_out, read_weights, memory_gate, write_pos):
    vm, hb = pl.BlockSpec(memory_space=pltpu.VMEM), pl.BlockSpec(memory_space=pltpu.HBM)
    V, D = pltpu.VMEM, pltpu.SemaphoreType.DMA
    scratch = [
        V((T, DS), BF16), V((2048, HS), BF16), V((MEM, T), F32), V((MEM, MEM), F32),
        V((1, MEM), jnp.int32),
        V((3, T, DS), BF16), V((2, T, HS), BF16), V((2048, HS), BF16),
        V((2, MEM, DS + 128), F32), V((4, MEM, DS + 128), F32), V((8, MEM, DS + 128), F32),
        V((MEM, DS), F32), V((4, 2 * MEM, DS), BF16), V((2, 2 * MEM, HS), BF16),
        V((2, T, HS), F32), V((T, HS), BF16), V((T, HS), BF16),
        V((4, 2, DS, HS), F32), V((4, 2, 256, HS), BF16), V((4, 2, 256, HS), BF16),
        V((4, 2, 256, HS), BF16), V((8, 256, HS), BF16), V((4, 64, HS), BF16), V((4, 64, HS), BF16),
        V((T, MEM), BF16),
        D((9,)), D((2, XCH)), D((2, XCH)), D((2, XCH)), D((2, XCH)), D((YCH,)), D((YCH,)),
        D((2,)), D((8,)), D((8,)), D((2,)), D((2,)), D((4,)), D((4,)), D((8,)), D((8,)),
        D((4,)), D((4,)), D((YCH,)), D((YCH,)),
        D((4, 2)), D((4, 2)), D((4, 2)), D((8,)), D((4,)), D((4,)),
    ]
    shapes = (
        jax.ShapeDtypeStruct((T, HS), BF16),
        jax.ShapeDtypeStruct((64, HS), F32),
        jax.ShapeDtypeStruct((MEM, DS), F32),
    )
    results = pl.pallas_call(
        kernel,
        out_shape=shapes,
        in_specs=[hb] * 6,
        out_specs=(vm,) * 3,
        scratch_shapes=scratch,
        compiler_params=pltpu.CompilerParams(
            collective_id=0, has_side_effects=True, vmem_limit_bytes=40 * 1024 * 1024
        ),
    )(*[
        pltpu.with_memory_space_constraint(v, pltpu.HBM)
        for v in (grad_out, attn_out, out_proj_t, read_weights.T, memory_gate, write_pos)
    ])
    return pl.pallas_call(
        finish,
        out_shape=shapes,
        in_specs=[vm] * 3,
        out_specs=(vm,) * 3,
        compiler_params=pltpu.CompilerParams(vmem_limit_bytes=8 * 1024 * 1024),
    )(*results)


def solution(mesh):
    placed = (
        P("dp", "tensor"), P(None, "tensor"), P("dp", "tensor"),
        P("dp", None), P("dp", None), P("dp", None),
    )
    return jax.shard_map(
        body, mesh=mesh, in_specs=placed,
        out_specs=(P("dp", "tensor"), P("dp", "tensor"), P("dp", "tensor")), check_vma=False,
    )
```

```python
import functools

import jax
import jax.numpy as jnp
from jax import lax
from jax.experimental import pallas as pl
from jax.experimental.pallas import tpu as pltpu
from jax.sharding import PartitionSpec as P

T, DS, HS, MEM = 768, 512, 256, 16
XCH, XROWS = 3, 256
YCH, YROWS = 3, 256
F32, BF16 = jnp.float32, jnp.bfloat16
HIGH = lax.Precision.HIGHEST
SUM0 = (((0,), (0,)), ((), ()))


def tdot(a, b, precision=None):
    return lax.dot_general(a, b, SUM0, precision=precision, preferred_element_type=F32)


def dot(a, b):
    return jnp.dot(a, b, preferred_element_type=F32)


def parts3(v):
    hi = v.astype(BF16)
    rest = v - hi.astype(F32)
    mid = rest.astype(BF16)
    return hi, mid, (rest - mid.astype(F32)).astype(BF16)


def apply_map(m, v):
    out = m[:, 0:1] * v[0:1, :]
    for k in range(1, MEM):
        out = out + m[:, k : k + 1] * v[k : k + 1, :]
    return out


def kernel(
    g_in, attn, w_in, rwt_in, gate_in, wp_in, oa, ow, om,
    g, w, rwt, gate, wp, G, A, WP, S1, S2, S3, vr, R, Rows, acc, Ps, Pr, Pf, Cs, Cr, Ss, Zr, Ys, Yr, oh,
    ins, xs, xr, fs, fr, ats, atr, w1, wzs, wzr, wc, l1, l2s, l2r, l3s, l3r, rs, rr,
    ps, pr, cs, cr, zs, zr, ys, yr, ygo,
):
    dp, tp = lax.axis_index("dp"), lax.axis_index("tensor")
    z, yl, c = lax.div(dp, 8), lax.rem(lax.div(dp, 2), 4), lax.rem(dp, 2)
    x, yh = lax.div(tp, 2), lax.rem(tp, 2)
    y = 4 * yh + yl

    def dev(x_=None, y_=None, z_=None, c_=None):
        x_ = x if x_ is None else x_
        y_ = y if y_ is None else y_
        z_ = z if z_ is None else z_
        c_ = c if c_ is None else c_
        return (8 * z_ + 2 * lax.rem(y_, 4) + c_, 2 * x_ + lax.div(y_, 4))

    def copy(src, dst, send, recv, to):
        return pltpu.make_async_remote_copy(
            src_ref=src, dst_ref=dst, send_sem=send, recv_sem=recv,
            device_id=to, device_id_type=pl.DeviceIdType.MESH,
        )

    xn = [lax.rem(x + k, 4) for k in range(4)]
    right, left, across = dev(x_=xn[1]), dev(x_=xn[3]), dev(x_=xn[2])
    yn = [lax.rem(y + k, 8) for k in range(8)]
    far = dev(y_=yn[4])
    ring = [dev(y_=yn[k]) for k in range(1, 8)]
    mate = dev(c_=1 - c)
    lo = [dev(y_=4 * yh + lax.rem(yl + k, 4)) for k in range(4)]
    zn = [lax.rem(z + k, 8) for k in range(8)]
    zdev = [dev(z_=zn[k]) for k in range(8)]
    odd = lax.rem(z, 2)
    zx = z + 1 - 2 * odd
    straight = odd == yh
    cross = [dev(y_=yn[k], z_=zx) for k in range(8)]

    barrier = pltpu.get_barrier_semaphore()
    greeted = [right, left, across, mate] + ring + zdev[1:] + cross
    for peer in greeted:
        pl.semaphore_signal(barrier, inc=1, device_id=peer, device_id_type=pl.DeviceIdType.MESH)

    loads = [
        pltpu.make_async_copy(wp_in, wp, ins.at[6]),
        pltpu.make_async_copy(gate_in, gate, ins.at[7]),
        pltpu.make_async_copy(rwt_in, rwt, ins.at[8]),
        pltpu.make_async_copy(g_in, g, ins.at[0]),
        pltpu.make_async_copy(attn, A.at[0], ins.at[1]),
    ]
    for k in range(4):
        block = pl.ds(pl.multiple_of((2 * k + yh) * DS, DS), DS)
        loads.append(pltpu.make_async_copy(w_in.at[block], w.at[pl.ds(k * DS, DS)], ins.at[2 + k]))
    for load in loads:
        load.start()

    loads[0].wait()
    picks = lax.broadcasted_iota(jnp.int32, (T, MEM), 0) == wp[...]
    oh[...] = picks.astype(F32).astype(BF16)
    eye = (
        lax.broadcasted_iota(jnp.int32, (MEM, 128), 0)
        == lax.broadcasted_iota(jnp.int32, (MEM, 128), 1)
    ).astype(F32)
    loads[1].wait()
    S1[c, :, DS:] = tdot(gate[...], eye, HIGH)
    loads[2].wait()
    hi, mid, low = parts3(rwt[...])
    loads[3].wait()
    gv = g[...]
    S1[c, :, :DS] = dot(low, gv) + dot(mid, gv) + dot(hi, gv)
    pl.semaphore_wait(barrier, len(greeted))

    sent = []

    def go(d):
        d.start()
        sent.append(d)

    lcopy = copy(S1.at[c], S1.at[c], l1.at[0], l1.at[1], mate)
    go(lcopy)

    def own_right(k):
        r = pl.ds(k * XROWS, XROWS)
        return copy(g.at[r], G.at[2, r], xs.at[0, k], xr.at[0, k], right)

    def own_left(k):
        r = pl.ds(k * XROWS, XROWS)
        return copy(g.at[r], G.at[0, r], xs.at[1, k], xr.at[1, k], left)

    half = XROWS // 2

    def on_right(k):
        r = pl.ds(k * XROWS, half)
        return copy(G.at[2, r], G.at[1, r], fs.at[0, k], fr.at[0, k], right)

    def on_left(k):
        r = pl.ds(k * XROWS + half, half)
        return copy(G.at[0, r], G.at[1, r], fs.at[1, k], fr.at[1, k], left)

    def attn_far(j):
        r = pl.ds(j * YROWS, YROWS)
        return copy(A.at[0, r], A.at[1, r], ats.at[j], atr.at[j], far)

    part = lax.rem(z, 4)
    wrow = pl.multiple_of(
        (2 * (2 * c + lax.div(part, 2)) + 1 - yh) * DS + lax.rem(part, 2) * 256, 256
    )

    def wpart(k):
        return pl.ds(pl.multiple_of(c * 1024 + lax.rem(z + k, 4) * 256, 256), 256)

    wfirst = copy(w_in.at[pl.ds(wrow, 256)], WP.at[wpart(0)], w1.at[0], w1.at[1], far)

    def compose(early, late):
        both = apply_map(early[:, DS:], late)
        return both[:, :DS] + early[:, :DS], both[:, DS:]

    lcopy.wait_recv()
    term, mat = compose(S1[0], S1[1])
    S2[yl, :, :DS] = term
    S2[yl, :, DS:] = mat
    for k in range(1, 4):
        go(copy(S2.at[yl], S2.at[yl], l2s.at[k], l2r.at[yl], lo[k]))
    loads[4].wait()
    go(wfirst)
    for k in range(XCH):
        go(own_right(k))
        go(own_left(k))
    grows = tdot(oh[...], gv)
    for k in range(1, 4):
        slot = lax.rem(yl + k, 4)
        copy(S2.at[slot], S2.at[slot], l2s.at[k], l2r.at[slot], lo[k]).wait_recv()
    for k in range(1, 8):
        pl.semaphore_signal(
            ygo, inc=1, device_id=ring[k - 1], device_id_type=pl.DeviceIdType.MESH
        )
    term, mat = compose(S2[2], S2[3])
    for k in (1, 0):
        term, mat = compose(S2[k], jnp.concatenate([term, mat], axis=1))
    S3[z, :, :DS] = term
    S3[z, :, DS:] = mat
    for zz in range(7):
        @pl.when(zz < z)
        def _():
            copy(S3.at[z], S3.at[z], l3s.at[zz], l3r.at[z], dev(z_=zz)).start()


    pl.semaphore_wait(ygo, 7)
    for j in range(YCH):
        go(attn_far(j))
    wfirst.wait_recv()

    wto = [zdev[1], zdev[7], dev(z_=lax.rem(z + 2 + 4 * c, 8))]

    def wspread(k, piece):
        return copy(WP.at[wpart(piece)], WP.at[wpart(piece)], wzs.at[k], wzr.at[k], wto[k])

    for k in range(3):
        go(wspread(k, 0))
    vr[...] = jnp.zeros((MEM, DS), F32)

    def through(s):
        vr[...] = apply_map(s[:, DS:], vr[...]) + s[:, :DS]

    for zz in range(7, 0, -1):
        @pl.when(zz > z)
        def _():
            copy(S3.at[zz], S3.at[zz], l3s.at[0], l3r.at[zz], dev(z_=zz)).wait_recv()
            through(S3[zz])

    for k in range(3, 0, -1):
        @pl.when(k > yl)
        def _():
            through(S2[k])

    @pl.when(c == 0)
    def _():
        through(S1[1])

    after = vr[...]
    mine = S1[c]
    om[...] = apply_map(mine[:, DS:], after) + mine[:, :DS]
    R[0, :MEM] = (grows + after).astype(BF16)
    R[0, MEM:] = (-grows).astype(BF16)

    def rcopy(k):
        return copy(R.at[0], R.at[4 - k], rs.at[k], rr.at[4 - k], (right, across, left)[k - 1])

    for k in (1, 3, 2):
        go(rcopy(k))
    def rows_of(rel):
        return g if rel == 0 else G.at[rel - 1]

    def forward(rel, which, first):
        src = rows_of(rel)
        if which == 0:
            weight = w[pl.ds(pl.multiple_of(xn[rel] * DS, DS), DS), :]
        else:
            weight = WP[pl.ds(pl.multiple_of(xn[rel] * DS, DS), DS), :]
        for b in range(3):
            r = pl.ds(b * 256, 256)
            part = dot(src[r, :], weight)
            acc[which, r, :] = part if first else acc[which, r, :] + part

    qs = (yh, 1 - yh)

    def gradient(rel, h):
        src = rows_of(rel)
        for b in range(2):
            cols = pl.ds(b * 256, 256)
            Pf[rel, h, cols, :] = tdot(src[:, cols], A[h]) + tdot(R[rel, :, cols], Rows[h])
        for k in range(4):
            theirs = pl.ds(pl.multiple_of((2 * k + 1 - c) * 64, 64), 64)
            Cs[rel, h, k * 64 : k * 64 + 64, :] = Pf[rel, h, theirs, :].astype(BF16)
        go(ccopy(rel, h))

    def ccopy(rel, h):
        return copy(Cs.at[rel, h], Cr.at[rel, h], cs.at[rel, h], cr.at[rel, h], mate)

    def zto(rel, h, r):
        return 2 * xn[rel] + (qs[h] if r == 0 else 1 - qs[h])

    def zsend(rel, h, r):
        rows = pl.ds(r * 128, 128)
        to = dev(z_=zto(rel, h, r))
        return copy(Ss.at[rel, h, rows], Zr.at[z, r], zs.at[rel, h, r], zr.at[z, r], to)

    def scatter(rel, h):
        ccopy(rel, h).wait_recv()
        for k in range(4):
            ours = pl.ds(pl.multiple_of((2 * k + c) * 64, 64), 64)
            part = slice(k * 64, k * 64 + 64)
            total = Pf[rel, h, ours, :] + Cr[rel, h, part, :].astype(F32)
            Ss[rel, h, part, :] = total.astype(BF16)
        for r in range(2):
            @pl.when(zto(rel, h, r) != z)
            def _():
                zsend(rel, h, r).start()

            @pl.when(zto(rel, h, r) == z)
            def _():
                Zr[z, r] = Ss[rel, h, r * 128 : r * 128 + 128, :]

    def pick(h):
        arows = tdot(oh[...], A[h]).astype(BF16)
        Rows[h, :MEM] = arows
        Rows[h, MEM:] = arows

    pick(0)
    gradient(0, 0)
    for k in range(XCH):
        own_right(k).wait_recv()
        go(on_right(k))
        own_left(k).wait_recv()
        go(on_left(k))
    rcopy(1).wait_recv()
    gradient(3, 0)
    rcopy(3).wait_recv()
    gradient(1, 0)
    for k, piece in enumerate((3, 1, 2)):
        wspread(k, piece).wait_recv()
    chalf = pl.ds(pl.multiple_of(c * 1024, 1024), 1024)
    ohalf = pl.ds(pl.multiple_of((1 - c) * 1024, 1024), 1024)
    go(copy(WP.at[chalf], WP.at[chalf], wc.at[0], wc.at[1], mate))
    scatter(0, 0)
    scatter(3, 0)
    scatter(1, 0)
    for load in loads[5:]:
        load.wait()
    for rel in (0, 3, 1):
        forward(rel, 0, rel == 0)
    copy(WP.at[ohalf], WP.at[ohalf], wc.at[0], wc.at[1], mate).wait_recv()
    for rel in (0, 3, 1):
        forward(rel, 1, rel == 0)
    rcopy(2).wait_recv()

    def change(which):
        total = None
        for rel in range(4):
            if which == 0:
                weight = w[pl.ds(pl.multiple_of(xn[rel] * DS, DS), DS), :]
            else:
                weight = WP[pl.ds(pl.multiple_of(xn[rel] * DS, DS), DS), :]
            part = dot(R[rel], weight)
            total = part if total is None else total + part
        return parts3(total[:MEM] + total[MEM:])

    def spread(rows, change3):
        o = oh[rows, :]
        return dot(o, change3[0]) + dot(o, change3[1]) + dot(o, change3[2])

    def part_far(j):
        r = pl.ds(j * YROWS, YROWS)
        return copy(Ps.at[r], Pr.at[r], ps.at[j], pr.at[j], far)

    theirs = change(1)
    weight = WP[pl.ds(pl.multiple_of(xn[2] * DS, DS), DS), :]
    for j in range(YCH):
        on_right(j).wait_recv()
        on_left(j).wait_recv()
        r = pl.ds(j * YROWS, YROWS)
        Ps[r, :] = (acc[1, r, :] + dot(G[1, r, :], weight) + spread(r, theirs)).astype(BF16)
        go(part_far(j))
    gradient(2, 0)
    forward(2, 0, False)
    scatter(2, 0)
    for j in range(YCH):
        attn_far(j).wait_recv()
    pick(1)
    gradient(0, 1)
    gradient(3, 1)
    scatter(0, 1)
    gradient(1, 1)
    scatter(3, 1)
    gradient(2, 1)
    scatter(1, 1)
    scatter(2, 1)
    ours = change(0)
    for j in range(YCH):
        r = pl.ds(j * YROWS, YROWS)
        acc[0, r, :] = acc[0, r, :] + spread(r, ours)
    for zz in range(8):
        @pl.when(zz != z)
        def _():
            for r in range(2):
                copy(
                    Zr.at[zz, r], Zr.at[zz, r], zs.at[0, 0, r], zr.at[zz, r], dev(z_=zz)
                ).wait_recv()

    total = Zr[0].astype(F32)
    for zz in range(1, 8):
        total = total + Zr[zz].astype(F32)
    for k in range(4):
        Ys[k] = total[k // 2, k % 2 * 64 : k % 2 * 64 + 64].astype(BF16)

    zf = z - odd + yh

    def ysend(k):
        there = dev(y_=4 * (odd if k < 2 else 1 - odd) + k, z_=zf)
        return copy(Ys.at[k], Yr.at[yl], ys.at[k], yr.at[yl], there)

    def stays(k):
        return jnp.logical_and(straight, yl == k)

    for k in range(4):
        if k < 2:
            @pl.when(stays(k))
            def _():
                Yr[k] = Ys[k]

            @pl.when(jnp.logical_not(stays(k)))
            def _():
                ysend(k).start()
        else:
            go(ysend(k))

    for j in range(YCH):
        part_far(j).wait_recv()
    oa[...] = (acc[0] + Pr[...].astype(F32)).astype(BF16)

    for k in range(4):
        come = copy(Ys.at[k], Yr.at[k], ys.at[k], yr.at[k], mate)
        if k < 2:
            @pl.when(jnp.logical_not(stays(k)))
            def _():
                come.wait_recv()
                come.wait_send()
        else:
            come.wait_recv()

    ow[...] = (Yr[0].astype(F32) + Yr[1].astype(F32)) + (Yr[2].astype(F32) + Yr[3].astype(F32))

    for d in sent:
        d.wait_send()
    for zz in range(7):
        @pl.when(zz < z)
        def _():
            copy(S3.at[z], S3.at[z], l3s.at[zz], l3r.at[z], dev(z_=zz)).wait_send()
    for rel in range(4):
        for h in range(2):
            for r in range(2):
                @pl.when(zto(rel, h, r) != z)
                def _():
                    zsend(rel, h, r).wait_send()


def finish(a, b, c, oa, ow, om):
    oa[...] = a[...]
    ow[...] = b[...]
    om[...] = c[...]


def body(attn_out, out_proj_t, grad_out, read_weights, memory_gate, write_pos):
    vm, hb = pl.BlockSpec(memory_space=pltpu.VMEM), pl.BlockSpec(memory_space=pltpu.HBM)
    V, D = pltpu.VMEM, pltpu.SemaphoreType.DMA
    scratch = [
        V((T, DS), BF16), V((2048, HS), BF16), V((MEM, T), F32), V((MEM, MEM), F32),
        V((1, MEM), jnp.int32),
        V((3, T, DS), BF16), V((2, T, HS), BF16), V((2048, HS), BF16),
        V((2, MEM, DS + 128), F32), V((4, MEM, DS + 128), F32), V((8, MEM, DS + 128), F32),
        V((MEM, DS), F32), V((4, 2 * MEM, DS), BF16), V((2, 2 * MEM, HS), BF16),
        V((2, T, HS), F32), V((T, HS), BF16), V((T, HS), BF16),
        V((4, 2, DS, HS), F32), V((4, 2, 256, HS), BF16), V((4, 2, 256, HS), BF16),
        V((4, 2, 256, HS), BF16), V((8, 2, 128, HS), BF16), V((4, 64, HS), BF16), V((4, 64, HS), BF16),
        V((T, MEM), BF16),
        D((9,)), D((2, XCH)), D((2, XCH)), D((2, XCH)), D((2, XCH)), D((YCH,)), D((YCH,)),
        D((2,)), D((8,)), D((8,)), D((2,)), D((2,)), D((4,)), D((4,)), D((8,)), D((8,)),
        D((4,)), D((4,)), D((YCH,)), D((YCH,)),
        D((4, 2)), D((4, 2)), D((4, 2, 2)), D((8, 2)), D((4,)), D((4,)), pltpu.SemaphoreType.REGULAR,
    ]
    shapes = (
        jax.ShapeDtypeStruct((T, HS), BF16),
        jax.ShapeDtypeStruct((64, HS), F32),
        jax.ShapeDtypeStruct((MEM, DS), F32),
    )
    results = pl.pallas_call(
        kernel,
        out_shape=shapes,
        in_specs=[hb] * 6,
        out_specs=(vm,) * 3,
        scratch_shapes=scratch,
        compiler_params=pltpu.CompilerParams(
            collective_id=0, has_side_effects=True, vmem_limit_bytes=40 * 1024 * 1024
        ),
    )(*[
        pltpu.with_memory_space_constraint(v, pltpu.HBM)
        for v in (grad_out, attn_out, out_proj_t, read_weights.T, memory_gate, write_pos)
    ])
    return pl.pallas_call(
        finish,
        out_shape=shapes,
        in_specs=[vm] * 3,
        out_specs=(vm,) * 3,
        compiler_params=pltpu.CompilerParams(vmem_limit_bytes=8 * 1024 * 1024),
    )(*results)


def solution(mesh):
    placed = (
        P("dp", "tensor"), P(None, "tensor"), P("dp", "tensor"),
        P("dp", None), P("dp", None), P("dp", None),
    )
    return jax.shard_map(
        body, mesh=mesh, in_specs=placed,
        out_specs=(P("dp", "tensor"), P("dp", "tensor"), P("dp", "tensor")), check_vma=False,
    )
```

```python
import functools

import jax
import jax.numpy as jnp
from jax import lax
from jax.experimental import pallas as pl
from jax.experimental.pallas import tpu as pltpu
from jax.sharding import PartitionSpec as P

T, DS, HS, MEM = 768, 512, 256, 16
HC = DS // 2
XCH, XROWS = 3, 256
YCH, YROWS = 3, 256
F32, BF16 = jnp.float32, jnp.bfloat16
HIGH = lax.Precision.HIGHEST
SUM0 = (((0,), (0,)), ((), ()))


def tdot(a, b, precision=None):
    return lax.dot_general(a, b, SUM0, precision=precision, preferred_element_type=F32)


def dot(a, b):
    return jnp.dot(a, b, preferred_element_type=F32)


def parts3(v):
    hi = v.astype(BF16)
    rest = v - hi.astype(F32)
    mid = rest.astype(BF16)
    return hi, mid, (rest - mid.astype(F32)).astype(BF16)


def apply_map(m, v):
    out = m[:, 0:1] * v[0:1, :]
    for k in range(1, MEM):
        out = out + m[:, k : k + 1] * v[k : k + 1, :]
    return out


def kernel(
    g_in, attn, w_in, rwt_in, gate_in, wp_in, oa, ow, om,
    g, w, rwt, gate, wp, G, A, WP, S1, S2, S3, vr, Sx, Lo, Vx, Vr, Af, R, Rows, acc, Ps, Pr, Pf, Cs, Cr, Ss, Zr, Ys, Yr, oh,
    ins, xs, xr, fs, fr, ats, atr, w1, wzs, wzr, wc, l1, vs, l2s, l2r, l3s, l3r, rs, rr,
    ps, pr, cs, cr, zs, zr, ys, yr, ygo,
):
    dp, tp = lax.axis_index("dp"), lax.axis_index("tensor")
    z, yl, c = lax.div(dp, 8), lax.rem(lax.div(dp, 2), 4), lax.rem(dp, 2)
    x, yh = lax.div(tp, 2), lax.rem(tp, 2)
    y = 4 * yh + yl

    def dev(x_=None, y_=None, z_=None, c_=None):
        x_ = x if x_ is None else x_
        y_ = y if y_ is None else y_
        z_ = z if z_ is None else z_
        c_ = c if c_ is None else c_
        return (8 * z_ + 2 * lax.rem(y_, 4) + c_, 2 * x_ + lax.div(y_, 4))

    def copy(src, dst, send, recv, to):
        return pltpu.make_async_remote_copy(
            src_ref=src, dst_ref=dst, send_sem=send, recv_sem=recv,
            device_id=to, device_id_type=pl.DeviceIdType.MESH,
        )

    xn = [lax.rem(x + k, 4) for k in range(4)]
    right, left, across = dev(x_=xn[1]), dev(x_=xn[3]), dev(x_=xn[2])
    yn = [lax.rem(y + k, 8) for k in range(8)]
    far = dev(y_=yn[4])
    ring = [dev(y_=yn[k]) for k in range(1, 8)]
    mate = dev(c_=1 - c)
    lo = [dev(y_=4 * yh + lax.rem(yl + k, 4)) for k in range(4)]
    zn = [lax.rem(z + k, 8) for k in range(8)]
    zdev = [dev(z_=zn[k]) for k in range(8)]
    odd = lax.rem(z, 2)
    zx = z + 1 - 2 * odd
    straight = odd == yh
    cross = [dev(y_=yn[k], z_=zx) for k in range(8)]

    barrier = pltpu.get_barrier_semaphore()
    greeted = [right, left, across, mate] + ring + zdev[1:] + cross
    for peer in greeted:
        pl.semaphore_signal(barrier, inc=1, device_id=peer, device_id_type=pl.DeviceIdType.MESH)

    loads = [
        pltpu.make_async_copy(wp_in, wp, ins.at[6]),
        pltpu.make_async_copy(gate_in, gate, ins.at[7]),
        pltpu.make_async_copy(rwt_in, rwt, ins.at[8]),
        pltpu.make_async_copy(g_in, g, ins.at[0]),
        pltpu.make_async_copy(attn, A.at[0], ins.at[1]),
    ]
    for k in range(4):
        block = pl.ds(pl.multiple_of((2 * k + yh) * DS, DS), DS)
        loads.append(pltpu.make_async_copy(w_in.at[block], w.at[pl.ds(k * DS, DS)], ins.at[2 + k]))
    for load in loads:
        load.start()

    loads[0].wait()
    picks = lax.broadcasted_iota(jnp.int32, (T, MEM), 0) == wp[...]
    oh[...] = picks.astype(F32).astype(BF16)
    eye = (
        lax.broadcasted_iota(jnp.int32, (MEM, 128), 0)
        == lax.broadcasted_iota(jnp.int32, (MEM, 128), 1)
    ).astype(F32)
    loads[1].wait()
    mat = tdot(gate[...], eye, HIGH)
    S1[c, :, HC:] = mat
    Sx[:, HC:] = mat
    loads[2].wait()
    hi, mid, low = parts3(rwt[...])
    loads[3].wait()
    gv = g[...]
    Lo[...] = dot(low, gv) + dot(mid, gv) + dot(hi, gv)
    mycols = pl.ds(pl.multiple_of(c * HC, HC), HC)
    matecols = pl.ds(pl.multiple_of((1 - c) * HC, HC), HC)
    S1[c, :, :HC] = Lo[:, mycols]
    Sx[:, :HC] = Lo[:, matecols]
    pl.semaphore_wait(barrier, len(greeted))

    sent = []

    def go(d):
        d.start()
        sent.append(d)

    lcopy = copy(Sx, S1.at[c], l1.at[0], l1.at[1], mate)
    go(lcopy)

    def own_right(k):
        r = pl.ds(k * XROWS, XROWS)
        return copy(g.at[r], G.at[2, r], xs.at[0, k], xr.at[0, k], right)

    def own_left(k):
        r = pl.ds(k * XROWS, XROWS)
        return copy(g.at[r], G.at[0, r], xs.at[1, k], xr.at[1, k], left)

    half = XROWS // 2

    def on_right(k):
        r = pl.ds(k * XROWS, half)
        return copy(G.at[2, r], G.at[1, r], fs.at[0, k], fr.at[0, k], right)

    def on_left(k):
        r = pl.ds(k * XROWS + half, half)
        return copy(G.at[0, r], G.at[1, r], fs.at[1, k], fr.at[1, k], left)

    def attn_far(j):
        r = pl.ds(j * YROWS, YROWS)
        return copy(A.at[0, r], A.at[1, r], ats.at[j], atr.at[j], far)

    part = lax.rem(z, 4)
    wrow = pl.multiple_of(
        (2 * (2 * c + lax.div(part, 2)) + 1 - yh) * DS + lax.rem(part, 2) * 256, 256
    )

    def wpart(k):
        return pl.ds(pl.multiple_of(c * 1024 + lax.rem(z + k, 4) * 256, 256), 256)

    wfirst = copy(w_in.at[pl.ds(wrow, 256)], WP.at[wpart(0)], w1.at[0], w1.at[1], far)

    for k in range(XCH):
        go(own_right(k))
        go(own_left(k))

    def compose(early, late):
        both = apply_map(early[:, HC:], late)
        return both[:, :HC] + early[:, :HC], both[:, HC:]

    lcopy.wait_recv()
    term, mat = compose(S1[0], S1[1])
    S2[yl, :, :HC] = term
    S2[yl, :, HC:] = mat
    for k in range(1, 4):
        go(copy(S2.at[yl], S2.at[yl], l2s.at[k], l2r.at[yl], lo[k]))
    loads[4].wait()
    go(wfirst)
    grows = tdot(oh[...], gv)
    for k in range(1, 4):
        slot = lax.rem(yl + k, 4)
        copy(S2.at[slot], S2.at[slot], l2s.at[k], l2r.at[slot], lo[k]).wait_recv()
    for k in range(1, 8):
        pl.semaphore_signal(
            ygo, inc=1, device_id=ring[k - 1], device_id_type=pl.DeviceIdType.MESH
        )
    term, mat = compose(S2[2], S2[3])
    for k in (1, 0):
        term, mat = compose(S2[k], jnp.concatenate([term, mat], axis=1))
    S3[z, :, :HC] = term
    S3[z, :, HC:] = mat
    for zz in range(7):
        @pl.when(zz < z)
        def _():
            copy(S3.at[z], S3.at[z], l3s.at[zz], l3r.at[z], dev(z_=zz)).start()


    pl.semaphore_wait(ygo, 7)
    for j in range(YCH):
        go(attn_far(j))
    wfirst.wait_recv()

    wto = [zdev[1], zdev[7], dev(z_=lax.rem(z + 2 + 4 * c, 8))]

    def wspread(k, piece):
        return copy(WP.at[wpart(piece)], WP.at[wpart(piece)], wzs.at[k], wzr.at[k], wto[k])

    for k in range(3):
        go(wspread(k, 0))
    vr[...] = jnp.zeros((MEM, HC), F32)

    def through(s):
        vr[...] = apply_map(s[:, HC:], vr[...]) + s[:, :HC]

    for zz in range(7, 0, -1):
        @pl.when(zz > z)
        def _():
            copy(S3.at[zz], S3.at[zz], l3s.at[0], l3r.at[zz], dev(z_=zz)).wait_recv()
            through(S3[zz])

    for k in range(3, 0, -1):
        @pl.when(k > yl)
        def _():
            through(S2[k])

    inner = apply_map(S1[1, :, HC:], vr[...]) + S1[1, :, :HC]
    own = jnp.where(c == 0, inner, vr[...])
    Vx[...] = jnp.where(c == 0, vr[...], inner)
    vcopy = copy(Vx, Vr, vs.at[0], vs.at[1], mate)
    go(vcopy)
    Af[:, mycols] = own
    vcopy.wait_recv()
    Af[:, matecols] = Vr[...]
    after = Af[...]
    om[...] = apply_map(S1[c, :, HC:], after) + Lo[...]
    R[0, :MEM] = (grows + after).astype(BF16)
    R[0, MEM:] = (-grows).astype(BF16)

    def rcopy(k):
        return copy(R.at[0], R.at[4 - k], rs.at[k], rr.at[4 - k], (right, across, left)[k - 1])

    for k in (1, 3, 2):
        go(rcopy(k))
    def rows_of(rel):
        return g if rel == 0 else G.at[rel - 1]

    def forward(rel, which, first):
        src = rows_of(rel)
        if which == 0:
            weight = w[pl.ds(pl.multiple_of(xn[rel] * DS, DS), DS), :]
        else:
            weight = WP[pl.ds(pl.multiple_of(xn[rel] * DS, DS), DS), :]
        for b in range(3):
            r = pl.ds(b * 256, 256)
            part = dot(src[r, :], weight)
            acc[which, r, :] = part if first else acc[which, r, :] + part

    qs = (yh, 1 - yh)

    def gradient(rel, h):
        src = rows_of(rel)
        for b in range(2):
            cols = pl.ds(b * 256, 256)
            Pf[rel, h, cols, :] = tdot(src[:, cols], A[h]) + tdot(R[rel, :, cols], Rows[h])
        for k in range(4):
            theirs = pl.ds(pl.multiple_of((2 * k + 1 - c) * 64, 64), 64)
            Cs[rel, h, k * 64 : k * 64 + 64, :] = Pf[rel, h, theirs, :].astype(BF16)
        go(ccopy(rel, h))

    def ccopy(rel, h):
        return copy(Cs.at[rel, h], Cr.at[rel, h], cs.at[rel, h], cr.at[rel, h], mate)

    def zto(rel, h, r):
        return 2 * xn[rel] + (qs[h] if r == 0 else 1 - qs[h])

    def zsend(rel, h, r):
        rows = pl.ds(r * 128, 128)
        to = dev(z_=zto(rel, h, r))
        return copy(Ss.at[rel, h, rows], Zr.at[z, r], zs.at[rel, h, r], zr.at[z, r], to)

    def scatter(rel, h):
        ccopy(rel, h).wait_recv()
        for k in range(4):
            ours = pl.ds(pl.multiple_of((2 * k + c) * 64, 64), 64)
            part = slice(k * 64, k * 64 + 64)
            total = Pf[rel, h, ours, :] + Cr[rel, h, part, :].astype(F32)
            Ss[rel, h, part, :] = total.astype(BF16)
        for r in range(2):
            @pl.when(zto(rel, h, r) != z)
            def _():
                zsend(rel, h, r).start()

            @pl.when(zto(rel, h, r) == z)
            def _():
                Zr[z, r] = Ss[rel, h, r * 128 : r * 128 + 128, :]

    def pick(h):
        arows = tdot(oh[...], A[h]).astype(BF16)
        Rows[h, :MEM] = arows
        Rows[h, MEM:] = arows

    pick(0)
    gradient(0, 0)
    for k in range(XCH):
        own_right(k).wait_recv()
        go(on_right(k))
        own_left(k).wait_recv()
        go(on_left(k))
    rcopy(1).wait_recv()
    gradient(3, 0)
    rcopy(3).wait_recv()
    gradient(1, 0)
    for k, piece in enumerate((3, 1, 2)):
        wspread(k, piece).wait_recv()
    chalf = pl.ds(pl.multiple_of(c * 1024, 1024), 1024)
    ohalf = pl.ds(pl.multiple_of((1 - c) * 1024, 1024), 1024)
    go(copy(WP.at[chalf], WP.at[chalf], wc.at[0], wc.at[1], mate))
    scatter(0, 0)
    scatter(3, 0)
    scatter(1, 0)
    for load in loads[5:]:
        load.wait()
    for rel in (0, 3, 1):
        forward(rel, 0, rel == 0)
    copy(WP.at[ohalf], WP.at[ohalf], wc.at[0], wc.at[1], mate).wait_recv()
    for rel in (0, 3, 1):
        forward(rel, 1, rel == 0)
    rcopy(2).wait_recv()

    def change(which):
        total = None
        for rel in range(4):
            if which == 0:
                weight = w[pl.ds(pl.multiple_of(xn[rel] * DS, DS), DS), :]
            else:
                weight = WP[pl.ds(pl.multiple_of(xn[rel] * DS, DS), DS), :]
            part = dot(R[rel], weight)
            total = part if total is None else total + part
        return parts3(total[:MEM] + total[MEM:])

    def spread(rows, change3):
        o = oh[rows, :]
        return dot(o, change3[0]) + dot(o, change3[1]) + dot(o, change3[2])

    def part_far(j):
        r = pl.ds(j * YROWS, YROWS)
        return copy(Ps.at[r], Pr.at[r], ps.at[j], pr.at[j], far)

    theirs = change(1)
    weight = WP[pl.ds(pl.multiple_of(xn[2] * DS, DS), DS), :]
    for j in range(YCH):
        on_right(j).wait_recv()
        on_left(j).wait_recv()
        r = pl.ds(j * YROWS, YROWS)
        Ps[r, :] = (acc[1, r, :] + dot(G[1, r, :], weight) + spread(r, theirs)).astype(BF16)
        go(part_far(j))
    gradient(2, 0)
    forward(2, 0, False)
    scatter(2, 0)
    for j in range(YCH):
        attn_far(j).wait_recv()
    pick(1)
    gradient(0, 1)
    gradient(3, 1)
    scatter(0, 1)
    gradient(1, 1)
    scatter(3, 1)
    gradient(2, 1)
    scatter(1, 1)
    scatter(2, 1)
    ours = change(0)
    for j in range(YCH):
        r = pl.ds(j * YROWS, YROWS)
        acc[0, r, :] = acc[0, r, :] + spread(r, ours)
    for zz in range(8):
        @pl.when(zz != z)
        def _():
            for r in range(2):
                copy(
                    Zr.at[zz, r], Zr.at[zz, r], zs.at[0, 0, r], zr.at[zz, r], dev(z_=zz)
                ).wait_recv()

    total = Zr[0].astype(F32)
    for zz in range(1, 8):
        total = total + Zr[zz].astype(F32)
    for k in range(4):
        Ys[k] = total[k // 2, k % 2 * 64 : k % 2 * 64 + 64].astype(BF16)

    zf = z - odd + yh

    def ysend(k):
        there = dev(y_=4 * (odd if k < 2 else 1 - odd) + k, z_=zf)
        return copy(Ys.at[k], Yr.at[yl], ys.at[k], yr.at[yl], there)

    def stays(k):
        return jnp.logical_and(straight, yl == k)

    for k in range(4):
        if k < 2:
            @pl.when(stays(k))
            def _():
                Yr[k] = Ys[k]

            @pl.when(jnp.logical_not(stays(k)))
            def _():
                ysend(k).start()
        else:
            go(ysend(k))

    for j in range(YCH):
        part_far(j).wait_recv()
    oa[...] = (acc[0] + Pr[...].astype(F32)).astype(BF16)

    for k in range(4):
        come = copy(Ys.at[k], Yr.at[k], ys.at[k], yr.at[k], mate)
        if k < 2:
            @pl.when(jnp.logical_not(stays(k)))
            def _():
                come.wait_recv()
                come.wait_send()
        else:
            come.wait_recv()

    ow[...] = (Yr[0].astype(F32) + Yr[1].astype(F32)) + (Yr[2].astype(F32) + Yr[3].astype(F32))

    for d in sent:
        d.wait_send()
    for zz in range(7):
        @pl.when(zz < z)
        def _():
            copy(S3.at[z], S3.at[z], l3s.at[zz], l3r.at[z], dev(z_=zz)).wait_send()
    for rel in range(4):
        for h in range(2):
            for r in range(2):
                @pl.when(zto(rel, h, r) != z)
                def _():
                    zsend(rel, h, r).wait_send()


def finish(a, b, c, oa, ow, om):
    oa[...] = a[...]
    ow[...] = b[...]
    om[...] = c[...]


def body(attn_out, out_proj_t, grad_out, read_weights, memory_gate, write_pos):
    vm, hb = pl.BlockSpec(memory_space=pltpu.VMEM), pl.BlockSpec(memory_space=pltpu.HBM)
    V, D = pltpu.VMEM, pltpu.SemaphoreType.DMA
    scratch = [
        V((T, DS), BF16), V((2048, HS), BF16), V((MEM, T), F32), V((MEM, MEM), F32),
        V((1, MEM), jnp.int32),
        V((3, T, DS), BF16), V((2, T, HS), BF16), V((2048, HS), BF16),
        V((2, MEM, HC + 128), F32), V((4, MEM, HC + 128), F32), V((8, MEM, HC + 128), F32),
        V((MEM, HC), F32), V((MEM, HC + 128), F32), V((MEM, DS), F32), V((MEM, HC), F32),
        V((MEM, HC), F32), V((MEM, DS), F32), V((4, 2 * MEM, DS), BF16), V((2, 2 * MEM, HS), BF16),
        V((2, T, HS), F32), V((T, HS), BF16), V((T, HS), BF16),
        V((4, 2, DS, HS), F32), V((4, 2, 256, HS), BF16), V((4, 2, 256, HS), BF16),
        V((4, 2, 256, HS), BF16), V((8, 2, 128, HS), BF16), V((4, 64, HS), BF16), V((4, 64, HS), BF16),
        V((T, MEM), BF16),
        D((9,)), D((2, XCH)), D((2, XCH)), D((2, XCH)), D((2, XCH)), D((YCH,)), D((YCH,)),
        D((2,)), D((8,)), D((8,)), D((2,)), D((2,)), D((2,)), D((4,)), D((4,)), D((8,)), D((8,)),
        D((4,)), D((4,)), D((YCH,)), D((YCH,)),
        D((4, 2)), D((4, 2)), D((4, 2, 2)), D((8, 2)), D((4,)), D((4,)), pltpu.SemaphoreType.REGULAR,
    ]
    shapes = (
        jax.ShapeDtypeStruct((T, HS), BF16),
        jax.ShapeDtypeStruct((64, HS), F32),
        jax.ShapeDtypeStruct((MEM, DS), F32),
    )
    results = pl.pallas_call(
        kernel,
        out_shape=shapes,
        in_specs=[hb] * 6,
        out_specs=(vm,) * 3,
        scratch_shapes=scratch,
        compiler_params=pltpu.CompilerParams(
            collective_id=0, has_side_effects=True, vmem_limit_bytes=40 * 1024 * 1024
        ),
    )(*[
        pltpu.with_memory_space_constraint(v, pltpu.HBM)
        for v in (grad_out, attn_out, out_proj_t, read_weights.T, memory_gate, write_pos)
    ])
    return pl.pallas_call(
        finish,
        out_shape=shapes,
        in_specs=[vm] * 3,
        out_specs=(vm,) * 3,
        compiler_params=pltpu.CompilerParams(vmem_limit_bytes=8 * 1024 * 1024),
    )(*results)


def solution(mesh):
    placed = (
        P("dp", "tensor"), P(None, "tensor"), P("dp", "tensor"),
        P("dp", None), P("dp", None), P("dp", None),
    )
    return jax.shard_map(
        body, mesh=mesh, in_specs=placed,
        out_specs=(P("dp", "tensor"), P("dp", "tensor"), P("dp", "tensor")), check_vma=False,
    )
```

```python
import functools

import jax
import jax.numpy as jnp
from jax import lax
from jax.experimental import pallas as pl
from jax.experimental.pallas import tpu as pltpu
from jax.sharding import PartitionSpec as P

T, DS, HS, MEM = 768, 512, 256, 16
HC = DS // 2
XCH, XROWS = 3, 256
YCH, YROWS = 3, 256
F32, BF16 = jnp.float32, jnp.bfloat16
HIGH = lax.Precision.HIGHEST
SUM0 = (((0,), (0,)), ((), ()))


def tdot(a, b, precision=None):
    return lax.dot_general(a, b, SUM0, precision=precision, preferred_element_type=F32)


def dot(a, b):
    return jnp.dot(a, b, preferred_element_type=F32)


def parts3(v):
    hi = v.astype(BF16)
    rest = v - hi.astype(F32)
    mid = rest.astype(BF16)
    return hi, mid, (rest - mid.astype(F32)).astype(BF16)


def apply_map(m, v):
    out = m[:, 0:1] * v[0:1, :]
    for k in range(1, MEM):
        out = out + m[:, k : k + 1] * v[k : k + 1, :]
    return out


def kernel(
    g_in, attn, w_in, rwt_in, gate_in, wp_in, oa, ow, om,
    g, w, rwt, gate, wp, G, A, WP, S1, S2, S3, vr, Sx, Lo, Vx, Vr, Af, R, Rows, acc, Ps, Pr, Pf, Cs, Cr, Ss, Zr, Ys, Yr, oh,
    ins, xs, xr, fs, fr, ats, atr, w1, wzs, wzr, wc, l1, vs, l2s, l2r, l3s, l3r, rs, rr,
    ps, pr, cs, cr, zs, zr, ys, yr, ygo,
):
    dp, tp = lax.axis_index("dp"), lax.axis_index("tensor")
    z, yl, c = lax.div(dp, 8), lax.rem(lax.div(dp, 2), 4), lax.rem(dp, 2)
    x, yh = lax.div(tp, 2), lax.rem(tp, 2)
    y = 4 * yh + yl

    def dev(x_=None, y_=None, z_=None, c_=None):
        x_ = x if x_ is None else x_
        y_ = y if y_ is None else y_
        z_ = z if z_ is None else z_
        c_ = c if c_ is None else c_
        return (8 * z_ + 2 * lax.rem(y_, 4) + c_, 2 * x_ + lax.div(y_, 4))

    def copy(src, dst, send, recv, to):
        return pltpu.make_async_remote_copy(
            src_ref=src, dst_ref=dst, send_sem=send, recv_sem=recv,
            device_id=to, device_id_type=pl.DeviceIdType.MESH,
        )

    xn = [lax.rem(x + k, 4) for k in range(4)]
    right, left, across = dev(x_=xn[1]), dev(x_=xn[3]), dev(x_=xn[2])
    yn = [lax.rem(y + k, 8) for k in range(8)]
    far = dev(y_=yn[4])
    ring = [dev(y_=yn[k]) for k in range(1, 8)]
    mate = dev(c_=1 - c)
    lo = [dev(y_=4 * yh + lax.rem(yl + k, 4)) for k in range(4)]
    zn = [lax.rem(z + k, 8) for k in range(8)]
    zdev = [dev(z_=zn[k]) for k in range(8)]
    odd = lax.rem(z, 2)
    zx = z + 1 - 2 * odd
    straight = odd == yh
    cross = [dev(y_=yn[k], z_=zx) for k in range(8)]

    barrier = pltpu.get_barrier_semaphore()
    greeted = [right, left, across, mate] + ring + zdev[1:] + cross
    for peer in greeted:
        pl.semaphore_signal(barrier, inc=1, device_id=peer, device_id_type=pl.DeviceIdType.MESH)

    loads = [
        pltpu.make_async_copy(wp_in, wp, ins.at[6]),
        pltpu.make_async_copy(gate_in, gate, ins.at[7]),
        pltpu.make_async_copy(rwt_in, rwt, ins.at[8]),
        pltpu.make_async_copy(g_in, g, ins.at[0]),
        pltpu.make_async_copy(attn, A.at[0], ins.at[1]),
    ]
    for k in range(4):
        block = pl.ds(pl.multiple_of((2 * k + yh) * DS, DS), DS)
        loads.append(pltpu.make_async_copy(w_in.at[block], w.at[pl.ds(k * DS, DS)], ins.at[2 + k]))
    for load in loads:
        load.start()

    loads[0].wait()
    picks = lax.broadcasted_iota(jnp.int32, (T, MEM), 0) == wp[...]
    oh[...] = picks.astype(F32).astype(BF16)
    eye = (
        lax.broadcasted_iota(jnp.int32, (MEM, 128), 0)
        == lax.broadcasted_iota(jnp.int32, (MEM, 128), 1)
    ).astype(F32)
    loads[1].wait()
    mat = tdot(gate[...], eye, HIGH)
    S1[c, :, HC:] = mat
    Sx[:, HC:] = mat
    loads[2].wait()
    hi, mid, low = parts3(rwt[...])
    loads[3].wait()
    gv = g[...]
    Lo[...] = dot(low, gv) + dot(mid, gv) + dot(hi, gv)
    mycols = pl.ds(pl.multiple_of(c * HC, HC), HC)
    matecols = pl.ds(pl.multiple_of((1 - c) * HC, HC), HC)
    S1[c, :, :HC] = Lo[:, mycols]
    Sx[:, :HC] = Lo[:, matecols]
    pl.semaphore_wait(barrier, len(greeted))

    sent = []

    def go(d):
        d.start()
        sent.append(d)

    lcopy = copy(Sx, S1.at[c], l1.at[0], l1.at[1], mate)
    go(lcopy)

    def own_right(k):
        r = pl.ds(k * XROWS, XROWS)
        return copy(g.at[r], G.at[2, r], xs.at[0, k], xr.at[0, k], right)

    def own_left(k):
        r = pl.ds(k * XROWS, XROWS)
        return copy(g.at[r], G.at[0, r], xs.at[1, k], xr.at[1, k], left)

    half = XROWS // 2

    def on_right(k):
        r = pl.ds(k * XROWS, half)
        return copy(G.at[2, r], G.at[1, r], fs.at[0, k], fr.at[0, k], right)

    def on_left(k):
        r = pl.ds(k * XROWS + half, half)
        return copy(G.at[0, r], G.at[1, r], fs.at[1, k], fr.at[1, k], left)

    def attn_far(j):
        r = pl.ds(j * YROWS, YROWS)
        return copy(A.at[0, r], A.at[1, r], ats.at[j], atr.at[j], far)

    part = lax.rem(z, 4)
    wrow = pl.multiple_of(
        (2 * (2 * c + lax.div(part, 2)) + 1 - yh) * DS + lax.rem(part, 2) * 256, 256
    )

    def wpart(k):
        return pl.ds(pl.multiple_of(c * 1024 + lax.rem(z + k, 4) * 256, 256), 256)

    wfirst = copy(w_in.at[pl.ds(wrow, 256)], WP.at[wpart(0)], w1.at[0], w1.at[1], far)

    for k in range(XCH):
        go(own_right(k))
        go(own_left(k))

    def compose(early, late):
        both = apply_map(early[:, HC:], late)
        return both[:, :HC] + early[:, :HC], both[:, HC:]

    lcopy.wait_recv()
    term, mat = compose(S1[0], S1[1])
    S2[yl, :, :HC] = term
    S2[yl, :, HC:] = mat
    for k in range(1, 4):
        go(copy(S2.at[yl], S2.at[yl], l2s.at[k], l2r.at[yl], lo[k]))
    loads[4].wait()
    go(wfirst)
    grows = tdot(oh[...], gv)
    for k in range(1, 4):
        slot = lax.rem(yl + k, 4)
        copy(S2.at[slot], S2.at[slot], l2s.at[k], l2r.at[slot], lo[k]).wait_recv()
    for k in range(1, 8):
        pl.semaphore_signal(
            ygo, inc=1, device_id=ring[k - 1], device_id_type=pl.DeviceIdType.MESH
        )
    term, mat = compose(S2[2], S2[3])
    for k in (1, 0):
        term, mat = compose(S2[k], jnp.concatenate([term, mat], axis=1))
    S3[z, :, :HC] = term
    S3[z, :, HC:] = mat
    for zz in range(7):
        @pl.when(zz < z)
        def _():
            copy(S3.at[z], S3.at[z], l3s.at[zz], l3r.at[z], dev(z_=zz)).start()


    pl.semaphore_wait(ygo, 7)
    for j in range(YCH):
        go(attn_far(j))
    wfirst.wait_recv()

    wto = [zdev[1], zdev[7], dev(z_=lax.rem(z + 2 + 4 * c, 8))]

    def wspread(k, piece):
        return copy(WP.at[wpart(piece)], WP.at[wpart(piece)], wzs.at[k], wzr.at[k], wto[k])

    for k in (2, 0, 1):
        go(wspread(k, 0))
    vr[...] = jnp.zeros((MEM, HC), F32)

    def through(s):
        vr[...] = apply_map(s[:, HC:], vr[...]) + s[:, :HC]

    for zz in range(7, 0, -1):
        @pl.when(zz > z)
        def _():
            copy(S3.at[zz], S3.at[zz], l3s.at[0], l3r.at[zz], dev(z_=zz)).wait_recv()
            through(S3[zz])

    for k in range(3, 0, -1):
        @pl.when(k > yl)
        def _():
            through(S2[k])

    inner = apply_map(S1[1, :, HC:], vr[...]) + S1[1, :, :HC]
    own = jnp.where(c == 0, inner, vr[...])
    Vx[...] = jnp.where(c == 0, vr[...], inner)
    vcopy = copy(Vx, Vr, vs.at[0], vs.at[1], mate)
    go(vcopy)
    Af[:, mycols] = own
    vcopy.wait_recv()
    Af[:, matecols] = Vr[...]
    after = Af[...]
    om[...] = apply_map(S1[c, :, HC:], after) + Lo[...]
    R[0, :MEM] = (grows + after).astype(BF16)
    R[0, MEM:] = (-grows).astype(BF16)

    def rcopy(k):
        return copy(R.at[0], R.at[4 - k], rs.at[k], rr.at[4 - k], (right, across, left)[k - 1])

    for k in (1, 3, 2):
        go(rcopy(k))
    def rows_of(rel):
        return g if rel == 0 else G.at[rel - 1]

    def forward(rel, which, first):
        src = rows_of(rel)
        if which == 0:
            weight = w[pl.ds(pl.multiple_of(xn[rel] * DS, DS), DS), :]
        else:
            weight = WP[pl.ds(pl.multiple_of(xn[rel] * DS, DS), DS), :]
        for b in range(3):
            r = pl.ds(b * 256, 256)
            part = dot(src[r, :], weight)
            acc[which, r, :] = part if first else acc[which, r, :] + part

    qs = (yh, 1 - yh)

    def gradient(rel, h):
        src = rows_of(rel)
        for b in range(2):
            cols = pl.ds(b * 256, 256)
            Pf[rel, h, cols, :] = tdot(src[:, cols], A[h]) + tdot(R[rel, :, cols], Rows[h])
        for k in range(4):
            theirs = pl.ds(pl.multiple_of((2 * k + 1 - c) * 64, 64), 64)
            Cs[rel, h, k * 64 : k * 64 + 64, :] = Pf[rel, h, theirs, :].astype(BF16)
        go(ccopy(rel, h))

    def ccopy(rel, h):
        return copy(Cs.at[rel, h], Cr.at[rel, h], cs.at[rel, h], cr.at[rel, h], mate)

    def zto(rel, h, r):
        return 2 * xn[rel] + (qs[h] if r == 0 else 1 - qs[h])

    def zsend(rel, h, r):
        rows = pl.ds(r * 128, 128)
        to = dev(z_=zto(rel, h, r))
        return copy(Ss.at[rel, h, rows], Zr.at[z, r], zs.at[rel, h, r], zr.at[z, r], to)

    def scatter(rel, h):
        ccopy(rel, h).wait_recv()
        for k in range(4):
            ours = pl.ds(pl.multiple_of((2 * k + c) * 64, 64), 64)
            part = slice(k * 64, k * 64 + 64)
            total = Pf[rel, h, ours, :] + Cr[rel, h, part, :].astype(F32)
            Ss[rel, h, part, :] = total.astype(BF16)
        for r in range(2):
            @pl.when(zto(rel, h, r) != z)
            def _():
                zsend(rel, h, r).start()

            @pl.when(zto(rel, h, r) == z)
            def _():
                Zr[z, r] = Ss[rel, h, r * 128 : r * 128 + 128, :]

    def pick(h):
        arows = tdot(oh[...], A[h]).astype(BF16)
        Rows[h, :MEM] = arows
        Rows[h, MEM:] = arows

    pick(0)
    gradient(0, 0)
    for k in range(XCH):
        own_right(k).wait_recv()
        go(on_right(k))
        own_left(k).wait_recv()
        go(on_left(k))
    scatter(0, 0)
    rcopy(1).wait_recv()
    gradient(3, 0)
    rcopy(3).wait_recv()
    gradient(1, 0)
    for k, piece in enumerate((3, 1, 2)):
        wspread(k, piece).wait_recv()
    chalf = pl.ds(pl.multiple_of(c * 1024, 1024), 1024)
    ohalf = pl.ds(pl.multiple_of((1 - c) * 1024, 1024), 1024)
    go(copy(WP.at[chalf], WP.at[chalf], wc.at[0], wc.at[1], mate))
    scatter(3, 0)
    scatter(1, 0)
    for load in loads[5:]:
        load.wait()
    for rel in (0, 3, 1):
        forward(rel, 0, rel == 0)
    copy(WP.at[ohalf], WP.at[ohalf], wc.at[0], wc.at[1], mate).wait_recv()
    for rel in (0, 3, 1):
        forward(rel, 1, rel == 0)
    rcopy(2).wait_recv()

    def change(which):
        total = None
        for rel in range(4):
            if which == 0:
                weight = w[pl.ds(pl.multiple_of(xn[rel] * DS, DS), DS), :]
            else:
                weight = WP[pl.ds(pl.multiple_of(xn[rel] * DS, DS), DS), :]
            part = dot(R[rel], weight)
            total = part if total is None else total + part
        return parts3(total[:MEM] + total[MEM:])

    def spread(rows, change3):
        o = oh[rows, :]
        return dot(o, change3[0]) + dot(o, change3[1]) + dot(o, change3[2])

    def part_far(j):
        r = pl.ds(j * YROWS, YROWS)
        return copy(Ps.at[r], Pr.at[r], ps.at[j], pr.at[j], far)

    theirs = change(1)
    weight = WP[pl.ds(pl.multiple_of(xn[2] * DS, DS), DS), :]
    for j in range(YCH):
        on_right(j).wait_recv()
        on_left(j).wait_recv()
        r = pl.ds(j * YROWS, YROWS)
        Ps[r, :] = (acc[1, r, :] + dot(G[1, r, :], weight) + spread(r, theirs)).astype(BF16)
        go(part_far(j))
    gradient(2, 0)
    forward(2, 0, False)
    scatter(2, 0)
    for j in range(YCH):
        attn_far(j).wait_recv()
    pick(1)
    gradient(0, 1)
    gradient(3, 1)
    scatter(0, 1)
    gradient(1, 1)
    scatter(3, 1)
    gradient(2, 1)
    scatter(1, 1)
    scatter(2, 1)
    ours = change(0)
    for j in range(YCH):
        r = pl.ds(j * YROWS, YROWS)
        acc[0, r, :] = acc[0, r, :] + spread(r, ours)
    for zz in range(8):
        @pl.when(zz != z)
        def _():
            for r in range(2):
                copy(
                    Zr.at[zz, r], Zr.at[zz, r], zs.at[0, 0, r], zr.at[zz, r], dev(z_=zz)
                ).wait_recv()

    total = Zr[0].astype(F32)
    for zz in range(1, 8):
        total = total + Zr[zz].astype(F32)
    for k in range(4):
        Ys[k] = total[k // 2, k % 2 * 64 : k % 2 * 64 + 64].astype(BF16)

    zf = z - odd + yh

    def ysend(k):
        there = dev(y_=4 * (odd if k < 2 else 1 - odd) + k, z_=zf)
        return copy(Ys.at[k], Yr.at[yl], ys.at[k], yr.at[yl], there)

    def stays(k):
        return jnp.logical_and(straight, yl == k)

    for k in range(4):
        if k < 2:
            @pl.when(stays(k))
            def _():
                Yr[k] = Ys[k]

            @pl.when(jnp.logical_not(stays(k)))
            def _():
                ysend(k).start()
        else:
            go(ysend(k))

    for j in range(YCH):
        part_far(j).wait_recv()
    oa[...] = (acc[0] + Pr[...].astype(F32)).astype(BF16)

    for k in range(4):
        come = copy(Ys.at[k], Yr.at[k], ys.at[k], yr.at[k], mate)
        if k < 2:
            @pl.when(jnp.logical_not(stays(k)))
            def _():
                come.wait_recv()
                come.wait_send()
        else:
            come.wait_recv()

    ow[...] = (Yr[0].astype(F32) + Yr[1].astype(F32)) + (Yr[2].astype(F32) + Yr[3].astype(F32))

    for d in sent:
        d.wait_send()
    for zz in range(7):
        @pl.when(zz < z)
        def _():
            copy(S3.at[z], S3.at[z], l3s.at[zz], l3r.at[z], dev(z_=zz)).wait_send()
    for rel in range(4):
        for h in range(2):
            for r in range(2):
                @pl.when(zto(rel, h, r) != z)
                def _():
                    zsend(rel, h, r).wait_send()


def finish(a, b, c, oa, ow, om):
    oa[...] = a[...]
    ow[...] = b[...]
    om[...] = c[...]


def body(attn_out, out_proj_t, grad_out, read_weights, memory_gate, write_pos):
    vm, hb = pl.BlockSpec(memory_space=pltpu.VMEM), pl.BlockSpec(memory_space=pltpu.HBM)
    V, D = pltpu.VMEM, pltpu.SemaphoreType.DMA
    scratch = [
        V((T, DS), BF16), V((2048, HS), BF16), V((MEM, T), F32), V((MEM, MEM), F32),
        V((1, MEM), jnp.int32),
        V((3, T, DS), BF16), V((2, T, HS), BF16), V((2048, HS), BF16),
        V((2, MEM, HC + 128), F32), V((4, MEM, HC + 128), F32), V((8, MEM, HC + 128), F32),
        V((MEM, HC), F32), V((MEM, HC + 128), F32), V((MEM, DS), F32), V((MEM, HC), F32),
        V((MEM, HC), F32), V((MEM, DS), F32), V((4, 2 * MEM, DS), BF16), V((2, 2 * MEM, HS), BF16),
        V((2, T, HS), F32), V((T, HS), BF16), V((T, HS), BF16),
        V((4, 2, DS, HS), F32), V((4, 2, 256, HS), BF16), V((4, 2, 256, HS), BF16),
        V((4, 2, 256, HS), BF16), V((8, 2, 128, HS), BF16), V((4, 64, HS), BF16), V((4, 64, HS), BF16),
        V((T, MEM), BF16),
        D((9,)), D((2, XCH)), D((2, XCH)), D((2, XCH)), D((2, XCH)), D((YCH,)), D((YCH,)),
        D((2,)), D((8,)), D((8,)), D((2,)), D((2,)), D((2,)), D((4,)), D((4,)), D((8,)), D((8,)),
        D((4,)), D((4,)), D((YCH,)), D((YCH,)),
        D((4, 2)), D((4, 2)), D((4, 2, 2)), D((8, 2)), D((4,)), D((4,)), pltpu.SemaphoreType.REGULAR,
    ]
    shapes = (
        jax.ShapeDtypeStruct((T, HS), BF16),
        jax.ShapeDtypeStruct((64, HS), F32),
        jax.ShapeDtypeStruct((MEM, DS), F32),
    )
    results = pl.pallas_call(
        kernel,
        out_shape=shapes,
        in_specs=[hb] * 6,
        out_specs=(vm,) * 3,
        scratch_shapes=scratch,
        compiler_params=pltpu.CompilerParams(
            collective_id=0, has_side_effects=True, vmem_limit_bytes=40 * 1024 * 1024
        ),
    )(*[
        pltpu.with_memory_space_constraint(v, pltpu.HBM)
        for v in (grad_out, attn_out, out_proj_t, read_weights.T, memory_gate, write_pos)
    ])
    return pl.pallas_call(
        finish,
        out_shape=shapes,
        in_specs=[vm] * 3,
        out_specs=(vm,) * 3,
        compiler_params=pltpu.CompilerParams(vmem_limit_bytes=8 * 1024 * 1024),
    )(*results)


def solution(mesh):
    placed = (
        P("dp", "tensor"), P(None, "tensor"), P("dp", "tensor"),
        P("dp", None), P("dp", None), P("dp", None),
    )
    return jax.shard_map(
        body, mesh=mesh, in_specs=placed,
        out_specs=(P("dp", "tensor"), P("dp", "tensor"), P("dp", "tensor")), check_vma=False,
    )
```
